128 devices in a mesh: section: 16 (over y_lo, x, core), tensor: 8 (over y_hi, z).
Axes of the slice: x: 4, y: 4 (y_hi: 2, y_lo: 2; y = y_hi * 2 + y_lo), z: 4, core: 2. Of those that a mesh axis runs over, the one named last changes fastest.
Arguments:
- key_weight: bfloat16 [16, 8192, 1024], P('section', None, 'tensor'), may hold values from -0.0625 to 0.0625
- value_weight: bfloat16 [16, 8192, 1024], P('section', None, 'tensor'), may hold values from -0.0625 to 0.0625
- norm_gain: bfloat16 [16, 8192], P('section'), may hold values from 0.25 to 1.75
Outputs:
- scaled: bfloat16 [16, 8192, 2048], P(None, ('section', 'tensor'))
- block_scale: float32 [16, 64, 16], P(None, 'section')
The draws below stay inside these ranges and needn't reach their ends.
All inputs are finite; a program needn't handle non-finite values.
Results may differ from the reference program's by a relative error of at most 0.0056.
Values may be sent and summed in bfloat16 or wider, within the bound.
A program may use at most 128 MiB of HBM per device.

```python
import jax
import jax.numpy as jnp
from jax import lax

D = 8192
BLOCK = 128
LAYERS = 16
KVW = 1024


def levels(own_key, extent, cuts, smallest, top_value):
    factor_of, own = 1.0, jax.random.fold_in(own_key, 6)
    for position, parts in cuts:
        draws = jnp.exp(jax.random.uniform(jax.random.fold_in(own, position), (parts,), jnp.float32, smallest / len(cuts), top_value / len(cuts)))
        factor_of = factor_of * jnp.repeat(draws, extent[position] // parts).reshape([-1 if axis == position else 1 for axis in range(len(extent))])
    return factor_of


def gaussian(own_key, extent, scale, reach, shards=(), held_as=jnp.bfloat16):
    result = jax.random.normal(own_key, extent, jnp.float32) * scale
    if len(shards) > 0:
        result = levels(own_key, extent, shards, -0.22, 0.18) * result
    return jnp.clip(result, min=-reach, max=reach).astype(held_as)


def setup_inputs(seed: int = 0) -> dict:
    splits = jax.random.split(jax.random.key(seed), 4)
    return {
        "key_weight": gaussian(splits[0], (LAYERS, D, KVW), D ** -0.5, 0.0625, ((0, 16), (2, 8))),
        "value_weight": gaussian(splits[1], (LAYERS, D, KVW), D ** -0.5, 0.0625, ((0, 16), (2, 8))),
        "norm_gain": jnp.clip(1.0 + 0.15 * jax.random.normal(splits[2], (LAYERS, D), jnp.float32), 0.25, 1.75).astype(jnp.bfloat16),
    }


scale_floor = 0.00390625


def quantize_layer(inputs):
    key_layer, value_layer, gain_layer = inputs
    stacked = jnp.concatenate([key_layer, value_layer], axis=1)
    folded = (gain_layer.astype(jnp.float32)[:, None] * stacked.astype(jnp.float32)).astype(jnp.bfloat16)
    folded = lax.optimization_barrier(folded).astype(jnp.float32)
    blocks = folded.reshape(D // BLOCK, BLOCK, 2 * KVW // BLOCK, BLOCK)
    block_max = jnp.max(jnp.abs(blocks), axis=(1, 3))
    block_scale = jnp.maximum(block_max, scale_floor)
    scaled = (blocks / block_scale[:, None, :, None]).astype(jnp.bfloat16).reshape(D, 2 * KVW)
    return scaled, block_scale


def reference(key_weight, value_weight, norm_gain):
    scaled, block_scale = lax.map(quantize_layer, (key_weight, value_weight, norm_gain))
    return scaled, block_scale
```

```python
import functools

import jax
import jax.numpy as jnp
from jax import lax
from jax.experimental import pallas as pl
from jax.experimental.pallas import tpu as pltpu
from jax.sharding import PartitionSpec as P

BLOCK = 128
SCALE_FLOOR = 0.00390625
MESH = pl.DeviceIdType.MESH


def exchange(
    sections, ranks, k_ref, v_ref, g_ref, out_ref, scale_ref,
    raw, gain, scaled, rows_out, rows_in,
    load_sem, gain_sem, send_sem, recv_sem, row_send_sem, row_recv_sem,
):
    devices = sections * ranks
    section, rank = lax.axis_index("section"), lax.axis_index("tensor")
    me = section * ranks + rank
    model_rows = k_ref.shape[1]
    part = model_rows // sections
    share = part // ranks
    blocks = part // BLOCK

    def section_at(step):
        across, low, core = step // 4, step // 2 % 2, step % 2
        shift = jnp.where(across == 0, 1, jnp.where(across == 1, 3, jnp.where(across == 2, 2, 0)))
        my_low, my_x, my_core = section // 8, section // 2 % 4, section % 2
        return (my_low + low) % 2 * 8 + (my_x + shift) % 4 * 2 + (my_core + core) % 2

    def loads(step):
        rows = pl.ds(pl.multiple_of(section_at(step) * part, part), part)
        return [
            pltpu.make_async_copy(ref.at[0, rows], raw.at[kind, rows], load_sem.at[step, kind])
            for kind, ref in enumerate((k_ref, v_ref))
        ]

    pltpu.make_async_copy(g_ref, gain, gain_sem).start()

    @pl.loop(0, sections)
    def _(step):
        for copy in loads(step):
            copy.start()

    barrier = pltpu.get_barrier_semaphore()

    @pl.loop(1, devices)
    def _(step):
        peer = lax.rem(me + step, devices)
        pl.semaphore_signal(
            barrier, inc=1, device_id=(peer // ranks, peer % ranks), device_id_type=MESH
        )

    pltpu.make_async_copy(g_ref, gain, gain_sem).wait()
    lanes = lax.broadcasted_iota(jnp.int32, (1, BLOCK), 1)

    def prepare(step):
        target = section_at(step)
        for copy in loads(step):
            copy.wait()
        row_values = jnp.zeros((1, BLOCK), jnp.float32)
        for block in range(blocks):
            start = pl.multiple_of(target * part + block * BLOCK, BLOCK)
            rows = pl.ds(start, BLOCK)
            gain_rows = jnp.broadcast_to(gain[:, rows].astype(jnp.float32), (BLOCK, BLOCK)).T
            for kind in range(2):
                folded = (gain_rows * raw[kind, rows, :].astype(jnp.float32)).astype(jnp.bfloat16)
                folded = folded.astype(jnp.float32)
                peak = jnp.max(jnp.abs(folded), axis=(0, 1), keepdims=True)
                peak = jnp.maximum(peak, SCALE_FLOOR)
                scaled[kind, rows, :] = (folded * (1.0 / peak)).astype(jnp.bfloat16)
                lane = (block * 2 + kind) * ranks + rank
                row_values = jnp.where(lanes == lane, peak, row_values)
        rows_out[target] = row_values
        return target

    def send(target, other):
        peer = target * ranks + other
        rows = pl.ds(pl.multiple_of(peer * share, share), share)
        columns = pl.ds(pl.multiple_of(rank * BLOCK, BLOCK), BLOCK)

        @pl.when(peer != me)
        def _():
            pltpu.make_async_remote_copy(
                src_ref=rows_out.at[target],
                dst_ref=rows_in.at[me],
                send_sem=row_send_sem,
                recv_sem=row_recv_sem,
                device_id=(target, other),
                device_id_type=MESH,
            ).start()
            pltpu.make_async_remote_copy(
                src_ref=scaled.at[:, rows],
                dst_ref=out_ref.at[section, :, :, columns],
                send_sem=send_sem,
                recv_sem=recv_sem.at[section],
                device_id=(target, other),
                device_id_type=MESH,
            ).start()

    first = prepare(0)
    pl.semaphore_wait(barrier, devices - 1)

    def send_all(target):
        @pl.loop(0, ranks)
        def _(step):
            send(target, lax.rem(rank + step + 1, ranks))

    send_all(first)

    @pl.loop(1, sections)
    def _(step):
        send_all(prepare(step))

    mine = pl.ds(pl.multiple_of(me * share, share), share)
    columns = pl.ds(pl.multiple_of(rank * BLOCK, BLOCK), BLOCK)
    out_ref[section, :, :, columns] = scaled[:, mine, :]
    rows_in[me] = rows_out[section]

    some_rows = rows_in.at[pl.ds(0, devices - 1)]
    pltpu.make_async_copy(some_rows, some_rows, row_recv_sem).wait()
    peaks = jnp.max(rows_in[...].reshape(sections, ranks, 1, BLOCK), axis=1)
    width = 2 * ranks
    for block in range(blocks):
        for layer in range(sections):
            scale_ref[layer, block : block + 1, :] = peaks[layer, :, block * width : (block + 1) * width]

    for layer in range(sections):

        @pl.when(layer != section)
        def _():
            whole = out_ref.at[layer]
            pltpu.make_async_copy(whole, whole, recv_sem.at[layer]).wait()

        @pl.when(layer == section)
        def _():
            most = out_ref.at[layer, :, :, pl.ds(0, (ranks - 1) * BLOCK)]
            pltpu.make_async_copy(most, most, recv_sem.at[layer]).wait()

    pltpu.make_async_copy(some_rows, some_rows, row_send_sem).wait()
    sent = scaled.at[:, pl.ds(0, (devices - 1) * share)]
    pltpu.make_async_copy(sent, sent, send_sem).wait()


def settle(wide_ref, narrow_ref, scaled_ref, scale_ref, sem, scale_sem):
    layers, kinds, _, columns = wide_ref.shape
    copies = [
        pltpu.make_async_copy(
            wide_ref.at[layer, kind],
            scaled_ref.at[layer, :, pl.ds(kind * columns, columns)],
            sem.at[layer, kind],
        )
        for layer in range(layers)
        for kind in range(kinds)
    ]
    copies.append(pltpu.make_async_copy(narrow_ref, scale_ref, scale_sem))
    for copy in copies:
        copy.start()
    for copy in copies:
        copy.wait()


def on_device(key_weight, value_weight, norm_gain):
    sections, ranks = lax.axis_size("section"), lax.axis_size("tensor")
    devices = sections * ranks
    model_rows = key_weight.shape[1]
    share = model_rows // devices
    blocks = model_rows // sections // BLOCK
    anywhere = pl.BlockSpec(memory_space=pl.ANY)
    in_vmem = pl.BlockSpec(memory_space=pltpu.VMEM)
    wide, narrow = pl.pallas_call(
        functools.partial(exchange, sections, ranks),
        out_shape=(
            pltpu.VMEM((sections, 2, share, ranks * BLOCK), jnp.bfloat16),
            pltpu.VMEM((sections, blocks, 2 * ranks), jnp.float32),
        ),
        in_specs=[anywhere] * 3,
        out_specs=(in_vmem, in_vmem),
        scratch_shapes=[
            pltpu.VMEM((2, model_rows, BLOCK), jnp.bfloat16),
            pltpu.VMEM((1, model_rows), jnp.bfloat16),
            pltpu.VMEM((2, model_rows, BLOCK), jnp.bfloat16),
            pltpu.VMEM((sections, 1, BLOCK), jnp.float32),
            pltpu.VMEM((devices, 1, BLOCK), jnp.float32),
            pltpu.SemaphoreType.DMA((sections, 2)),
            pltpu.SemaphoreType.DMA,
            pltpu.SemaphoreType.DMA,
            pltpu.SemaphoreType.DMA((sections,)),
            pltpu.SemaphoreType.DMA,
            pltpu.SemaphoreType.DMA,
        ],
        compiler_params=pltpu.CompilerParams(
            collective_id=0, has_side_effects=True, vmem_limit_bytes=32 * 1024 * 1024
        ),
    )(key_weight, value_weight, norm_gain)
    return pl.pallas_call(
        settle,
        out_shape=(
            jax.ShapeDtypeStruct((sections, share, 2 * ranks * BLOCK), jnp.bfloat16),
            jax.ShapeDtypeStruct(narrow.shape, jnp.float32),
        ),
        in_specs=[in_vmem, in_vmem],
        out_specs=(anywhere, anywhere),
        scratch_shapes=[
            pltpu.SemaphoreType.DMA((sections, 2)),
            pltpu.SemaphoreType.DMA,
        ],
    )(wide, narrow)


def solution(mesh):
    placed = (P("section", None, "tensor"), P("section", None, "tensor"), P("section", None))
    return jax.shard_map(
        on_device,
        mesh=mesh,
        in_specs=placed,
        out_specs=(P(None, ("section", "tensor"), None), P(None, "section", None)),
        check_vma=False,
    )
```

```python
import functools

import jax
import jax.numpy as jnp
from jax import lax
from jax.experimental import pallas as pl
from jax.experimental.pallas import tpu as pltpu
from jax.sharding import PartitionSpec as P

BLOCK = 128
SCALE_FLOOR = 0.00390625
MESH = pl.DeviceIdType.MESH


def exchange(
    sections, ranks, k_ref, v_ref, g_ref, out_ref, scale_ref,
    raw, gain, scaled, rows_out, rows_in,
    load_sem, gain_sem, send_sem, recv_sem, row_send_sem, row_recv_sem,
):
    devices = sections * ranks
    section, rank = lax.axis_index("section"), lax.axis_index("tensor")
    me = section * ranks + rank
    model_rows = k_ref.shape[1]
    part = model_rows // sections
    share = part // ranks
    blocks = part // BLOCK

    def section_at(step):
        across, low, core = step // 4, step // 2 % 2, step % 2
        shift = jnp.where(across == 0, 1, jnp.where(across == 1, 3, jnp.where(across == 2, 2, 0)))
        my_low, my_x, my_core = section // 8, section // 2 % 4, section % 2
        return (my_low + low) % 2 * 8 + (my_x + shift) % 4 * 2 + (my_core + core) % 2

    def loads(step):
        rows = pl.ds(pl.multiple_of(section_at(step) * part, part), part)
        return [
            pltpu.make_async_copy(ref.at[0, rows], raw.at[kind, rows], load_sem.at[step, kind])
            for kind, ref in enumerate((k_ref, v_ref))
        ]

    pltpu.make_async_copy(g_ref, gain, gain_sem).start()

    @pl.loop(0, sections)
    def _(step):
        for copy in loads(step):
            copy.start()

    barrier = pltpu.get_barrier_semaphore()

    @pl.loop(1, devices)
    def _(step):
        peer = lax.rem(me + step, devices)
        pl.semaphore_signal(
            barrier, inc=1, device_id=(peer // ranks, peer % ranks), device_id_type=MESH
        )

    pltpu.make_async_copy(g_ref, gain, gain_sem).wait()
    lanes = lax.broadcasted_iota(jnp.int32, (1, BLOCK), 1)

    def prepare(step):
        target = section_at(step)
        for copy in loads(step):
            copy.wait()
        row_values = jnp.zeros((1, BLOCK), jnp.float32)
        for block in range(blocks):
            start = pl.multiple_of(target * part + block * BLOCK, BLOCK)
            rows = pl.ds(start, BLOCK)
            gain_rows = jnp.broadcast_to(gain[:, rows].astype(jnp.float32), (BLOCK, BLOCK)).T
            for kind in range(2):
                folded = (gain_rows * raw[kind, rows, :].astype(jnp.float32)).astype(jnp.bfloat16)
                folded = folded.astype(jnp.float32)
                peak = jnp.max(jnp.abs(folded), axis=(0, 1), keepdims=True)
                peak = jnp.maximum(peak, SCALE_FLOOR)
                scaled[kind, rows, :] = (folded * (1.0 / peak)).astype(jnp.bfloat16)
                lane = (block * 2 + kind) * ranks + rank
                row_values = jnp.where(lanes == lane, peak, row_values)
        rows_out[target] = row_values
        return target

    def send(target, other):
        peer = target * ranks + other
        rows = pl.ds(pl.multiple_of(peer * share, share), share)
        columns = pl.ds(pl.multiple_of(rank * BLOCK, BLOCK), BLOCK)

        @pl.when(peer != me)
        def _():
            pltpu.make_async_remote_copy(
                src_ref=rows_out.at[target],
                dst_ref=rows_in.at[me],
                send_sem=row_send_sem,
                recv_sem=row_recv_sem,
                device_id=(target, other),
                device_id_type=MESH,
            ).start()
            pltpu.make_async_remote_copy(
                src_ref=scaled.at[:, rows],
                dst_ref=out_ref.at[section, :, :, columns],
                send_sem=send_sem,
                recv_sem=recv_sem.at[section],
                device_id=(target, other),
                device_id_type=MESH,
            ).start()

    first = prepare(0)
    pl.semaphore_wait(barrier, devices - 1)

    def send_all(target):
        @pl.loop(0, ranks)
        def _(step):
            send(target, lax.rem(rank + step + 1, ranks))

    send_all(first)

    @pl.loop(1, sections)
    def _(step):
        send_all(prepare(step))

    mine = pl.ds(pl.multiple_of(me * share, share), share)
    columns = pl.ds(pl.multiple_of(rank * BLOCK, BLOCK), BLOCK)
    out_ref[section, :, :, columns] = scaled[:, mine, :]
    rows_in[me] = rows_out[section]

    some_rows = rows_in.at[pl.ds(0, devices - 1)]
    pltpu.make_async_copy(some_rows, some_rows, row_recv_sem).wait()
    peaks = jnp.max(rows_in[...].reshape(sections, ranks, 1, BLOCK), axis=1)
    width = 2 * ranks
    for block in range(blocks):
        for layer in range(sections):
            scale_ref[layer, block : block + 1, :] = peaks[layer, :, block * width : (block + 1) * width]

    for layer in range(sections):

        @pl.when(layer != section)
        def _():
            whole = out_ref.at[layer]
            pltpu.make_async_copy(whole, whole, recv_sem.at[layer]).wait()

        @pl.when(layer == section)
        def _():
            most = out_ref.at[layer, :, :, pl.ds(0, (ranks - 1) * BLOCK)]
            pltpu.make_async_copy(most, most, recv_sem.at[layer]).wait()

    pltpu.make_async_copy(some_rows, some_rows, row_send_sem).wait()
    sent = scaled.at[:, pl.ds(0, (devices - 1) * share)]
    pltpu.make_async_copy(sent, sent, send_sem).wait()


def settle(wide_ref, narrow_ref, scaled_ref, scale_ref, sem, scale_sem):
    layers, kinds, _, columns = wide_ref.shape
    copies = [
        pltpu.make_async_copy(
            wide_ref.at[layer, kind],
            scaled_ref.at[layer, :, pl.ds(kind * columns, columns)],
            sem.at[layer, kind],
        )
        for layer in range(layers)
        for kind in range(kinds)
    ]
    copies.append(pltpu.make_async_copy(narrow_ref, scale_ref, scale_sem))
    for copy in copies:
        copy.start()
    for copy in copies:
        copy.wait()


def on_device(key_weight, value_weight, norm_gain):
    sections, ranks = lax.axis_size("section"), lax.axis_size("tensor")
    devices = sections * ranks
    model_rows = key_weight.shape[1]
    share = model_rows // devices
    blocks = model_rows // sections // BLOCK
    anywhere = pl.BlockSpec(memory_space=pl.ANY)
    in_vmem = pl.BlockSpec(memory_space=pltpu.VMEM)
    in_space = pltpu.with_memory_space_constraint
    wide, narrow = pl.pallas_call(
        functools.partial(exchange, sections, ranks),
        out_shape=(
            pltpu.VMEM((sections, 2, share, ranks * BLOCK), jnp.bfloat16),
            pltpu.VMEM((sections, blocks, 2 * ranks), jnp.float32),
        ),
        in_specs=[anywhere] * 3,
        out_specs=(in_vmem, in_vmem),
        scratch_shapes=[
            pltpu.VMEM((2, model_rows, BLOCK), jnp.bfloat16),
            pltpu.VMEM((1, model_rows), jnp.bfloat16),
            pltpu.VMEM((2, model_rows, BLOCK), jnp.bfloat16),
            pltpu.VMEM((sections, 1, BLOCK), jnp.float32),
            pltpu.VMEM((devices, 1, BLOCK), jnp.float32),
            pltpu.SemaphoreType.DMA((sections, 2)),
            pltpu.SemaphoreType.DMA,
            pltpu.SemaphoreType.DMA,
            pltpu.SemaphoreType.DMA((sections,)),
            pltpu.SemaphoreType.DMA,
            pltpu.SemaphoreType.DMA,
        ],
        compiler_params=pltpu.CompilerParams(
            collective_id=0, has_side_effects=True, vmem_limit_bytes=32 * 1024 * 1024
        ),
    )(*(in_space(array, pltpu.HBM) for array in (key_weight, value_weight, norm_gain)))
    return pl.pallas_call(
        settle,
        out_shape=(
            jax.ShapeDtypeStruct((sections, share, 2 * ranks * BLOCK), jnp.bfloat16),
            jax.ShapeDtypeStruct(narrow.shape, jnp.float32),
        ),
        in_specs=[in_vmem, in_vmem],
        out_specs=(anywhere, anywhere),
        scratch_shapes=[
            pltpu.SemaphoreType.DMA((sections, 2)),
            pltpu.SemaphoreType.DMA,
        ],
        compiler_params=pltpu.CompilerParams(vmem_limit_bytes=4 * 1024 * 1024),
    )(in_space(wide, pltpu.VMEM), in_space(narrow, pltpu.VMEM))


def solution(mesh):
    placed = (P("section", None, "tensor"), P("section", None, "tensor"), P("section", None))
    return jax.shard_map(
        on_device,
        mesh=mesh,
        in_specs=placed,
        out_specs=(P(None, ("section", "tensor"), None), P(None, "section", None)),
        check_vma=False,
    )
```

```python
import functools
import itertools

import jax
import jax.numpy as jnp
from jax import lax
from jax.experimental import pallas as pl
from jax.experimental.pallas import tpu as pltpu
from jax.sharding import PartitionSpec as P

BLOCK = 128
SCALE_FLOOR = 0.00390625
MESH = pl.DeviceIdType.MESH
SIDE = 4
CHUNK = 4
AHEAD = 3


def hops(offset):
    return sum(min(value, SIDE - value) for value in offset[:3])


def axes_used(offset):
    return sum(value != 0 for value in offset[:3])


def send_order():
    chips = list(itertools.product(range(SIDE), repeat=3))
    kind = {chip: tuple(sorted(min(v, SIDE - v) for v in chip)) for chip in chips}
    order = []
    for alike in sorted(set(kind.values()), key=lambda k: (-sum(k), k)):
        turn = []
        for chip in chips:
            if kind[chip] != alike:
                continue
            for shift in range(3):
                rolled = chip[-shift:] + chip[:-shift] if shift else chip
                for member in (rolled, tuple(-v % SIDE for v in rolled)):
                    if member not in turn:
                        turn.append(member)
        order += [member + (core,) for core in range(2) for member in turn]
    order.remove((0, 0, 0, 0))
    return order


ORDER = send_order()
LINES = [o for o in ORDER if axes_used(o) <= 1]
PLANES = [o for o in ORDER if axes_used(o) == 2]
REST = [o for o in ORDER if axes_used(o) == 3]


def block_of(offset):
    return offset[:2] + (offset[2] // 2, offset[3])


BLOCKS = list(dict.fromkeys(block_of(o) for o in LINES + PLANES + REST))
CHUNKS = [BLOCKS[i : i + CHUNK] for i in range(0, len(BLOCKS), CHUNK)]
PLACE = {block: (i // CHUNK, i % CHUNK) for i, block in enumerate(BLOCKS)}


def exchange(
    sections, ranks, k_ref, v_ref, g_ref, out_ref, scale_ref,
    raw, gain, scaled, rows_out, rows_in,
    load_sem, gain_sem, send_sem, recv_sem, row_send_sem, row_recv_sem, plane_sem, rest_sem,
):
    devices = sections * ranks
    section, rank = lax.axis_index("section"), lax.axis_index("tensor")
    me = section * ranks + rank
    model_rows = k_ref.shape[1]
    part = model_rows // sections
    share = part // ranks
    blocks = part // BLOCK
    core, my_x = section % 2, section // 2 % SIDE
    my_y, my_z = rank // SIDE * 2 + section // (2 * SIDE), rank % SIDE
    toward = 1 - 2 * (my_z % 2)

    def target(offset):
        x, y = (my_x + offset[0]) % SIDE, (my_y + offset[1]) % SIDE
        z = (my_z + toward * offset[2] + SIDE) % SIDE
        return (y % 2 * SIDE + x) * 2 + (core + offset[3]) % 2, y // 2 * SIDE + z

    def block_at(block):
        there, other = target(block[:2] + (block[2] * 2, block[3]))
        return there, other // 2

    def load(chunk):
        for place, block in enumerate(CHUNKS[chunk]):
            there, inner = block_at(block)
            rows = pl.ds(pl.multiple_of(there * part + inner * BLOCK, BLOCK), BLOCK)
            for kind, ref in enumerate((k_ref, v_ref)):
                pltpu.make_async_copy(
                    ref.at[0, rows], raw.at[chunk, kind, place], load_sem.at[chunk]
                ).start()

    lanes = lax.broadcasted_iota(jnp.int32, (1, BLOCK), 1)

    def compute(chunk):
        if chunk + AHEAD < len(CHUNKS):
            load(chunk + AHEAD)
        pltpu.make_async_copy(raw.at[chunk], raw.at[chunk], load_sem.at[chunk]).wait()
        for place, block in enumerate(CHUNKS[chunk]):
            there, inner = block_at(block)
            start = pl.multiple_of(there * part + inner * BLOCK, BLOCK)
            gain_rows = gain[:, pl.ds(start, BLOCK)].astype(jnp.float32)
            gain_rows = jnp.broadcast_to(gain_rows, (BLOCK, BLOCK)).T
            row_values = rows_out[there]
            for kind in range(2):
                folded = gain_rows * raw[chunk, kind, place].astype(jnp.float32)
                folded = folded.astype(jnp.bfloat16).astype(jnp.float32)
                peak = jnp.max(jnp.abs(folded), axis=(0, 1), keepdims=True)
                peak = jnp.maximum(peak, SCALE_FLOOR)
                scaled[chunk, place, kind] = (folded * (1.0 / peak)).astype(jnp.bfloat16)
                lane = (inner * 2 + kind) * ranks + rank
                row_values = jnp.where(lanes == lane, peak, row_values)
            rows_out[there] = row_values

    columns = pl.ds(pl.multiple_of(rank * BLOCK, BLOCK), BLOCK)

    def piece(offset):
        there, other = target(offset)
        chunk, place = PLACE[block_of(offset)]
        half = pl.multiple_of(other % 2 * share, share)
        return there, other, scaled.at[chunk, place, :, pl.ds(half, share)]

    def send(offset):
        there, other, source = piece(offset)
        pltpu.make_async_remote_copy(
            src_ref=source,
            dst_ref=out_ref.at[section, :, :, columns],
            send_sem=send_sem,
            recv_sem=recv_sem.at[section],
            device_id=(there, other),
            device_id_type=MESH,
        ).start()

    def greet(semaphore):
        for offset in LINES:
            pl.semaphore_signal(
                semaphore, inc=1, device_id=target(offset), device_id_type=MESH
            )

    done = 0

    def send_group(group, done):
        for offset in group:
            while PLACE[block_of(offset)][0] >= done:
                compute(done)
                done += 1
            send(offset)
        return done

    barrier = pltpu.get_barrier_semaphore()
    gain_copy = pltpu.make_async_copy(g_ref, gain, gain_sem)
    gain_copy.start()
    load(0)
    greet(barrier)
    for chunk in range(1, AHEAD):
        load(chunk)
    rows_out[...] = jnp.zeros_like(rows_out)
    gain_copy.wait()
    compute(0)
    done = 1
    pl.semaphore_wait(barrier, len(LINES))
    greet(plane_sem)
    done = send_group(LINES, done)
    pl.semaphore_wait(plane_sem, len(LINES))
    greet(rest_sem)
    done = send_group(PLANES, done)
    while done < len(CHUNKS):
        compute(done)
        done += 1
    pl.semaphore_wait(rest_sem, len(LINES))

    @pl.loop(1, devices)
    def _(step):
        peer = lax.rem(me + step, devices)
        there, other = peer // ranks, peer % ranks
        pltpu.make_async_remote_copy(
            src_ref=rows_out.at[there],
            dst_ref=rows_in.at[me],
            send_sem=row_send_sem,
            recv_sem=row_recv_sem,
            device_id=(there, other),
            device_id_type=MESH,
        ).start()

    send_group(REST, done)

    out_ref[section, :, :, columns] = piece((0, 0, 0, 0))[2][...]
    rows_in[me] = rows_out[section]

    some_rows = rows_in.at[pl.ds(0, devices - 1)]
    pltpu.make_async_copy(some_rows, some_rows, row_recv_sem).wait()
    peaks = jnp.max(rows_in[...].reshape(sections, ranks, 1, BLOCK), axis=1)
    width = 2 * ranks
    for block in range(blocks):
        for layer in range(sections):
            scale_ref[layer, block : block + 1, :] = peaks[layer, :, block * width : (block + 1) * width]

    for layer in range(sections):

        @pl.when(layer != section)
        def _():
            whole = out_ref.at[layer]
            pltpu.make_async_copy(whole, whole, recv_sem.at[layer]).wait()

        @pl.when(layer == section)
        def _():
            most = out_ref.at[layer, :, :, pl.ds(0, (ranks - 1) * BLOCK)]
            pltpu.make_async_copy(most, most, recv_sem.at[layer]).wait()

    pltpu.make_async_copy(some_rows, some_rows, row_send_sem).wait()
    half = scaled.at[0, 0, :, pl.ds(0, share)]
    all_but_one = scaled.at[pl.ds(0, len(CHUNKS) - 1)]
    pltpu.make_async_copy(all_but_one, all_but_one, send_sem).wait()
    last = scaled.at[0, pl.ds(0, CHUNK - 1)]
    pltpu.make_async_copy(last, last, send_sem).wait()
    pltpu.make_async_copy(half, half, send_sem).wait()


def settle(wide_ref, narrow_ref, scaled_ref, scale_ref, sem, scale_sem):
    layers, kinds, _, columns = wide_ref.shape
    copies = [
        pltpu.make_async_copy(
            wide_ref.at[layer, kind],
            scaled_ref.at[layer, :, pl.ds(kind * columns, columns)],
            sem.at[layer, kind],
        )
        for layer in range(layers)
        for kind in range(kinds)
    ]
    copies.append(pltpu.make_async_copy(narrow_ref, scale_ref, scale_sem))
    for copy in copies:
        copy.start()
    for copy in copies:
        copy.wait()


def on_device(key_weight, value_weight, norm_gain):
    sections, ranks = lax.axis_size("section"), lax.axis_size("tensor")
    devices = sections * ranks
    model_rows = key_weight.shape[1]
    share = model_rows // devices
    blocks = model_rows // sections // BLOCK
    anywhere = pl.BlockSpec(memory_space=pl.ANY)
    in_vmem = pl.BlockSpec(memory_space=pltpu.VMEM)
    in_space = pltpu.with_memory_space_constraint
    wide, narrow = pl.pallas_call(
        functools.partial(exchange, sections, ranks),
        out_shape=(
            pltpu.VMEM((sections, 2, share, ranks * BLOCK), jnp.bfloat16),
            pltpu.VMEM((sections, blocks, 2 * ranks), jnp.float32),
        ),
        in_specs=[anywhere] * 3,
        out_specs=(in_vmem, in_vmem),
        scratch_shapes=[
            pltpu.VMEM((len(CHUNKS), 2, CHUNK, BLOCK, BLOCK), jnp.bfloat16),
            pltpu.VMEM((1, model_rows), jnp.bfloat16),
            pltpu.VMEM((len(CHUNKS), CHUNK, 2, BLOCK, BLOCK), jnp.bfloat16),
            pltpu.VMEM((sections, 1, BLOCK), jnp.float32),
            pltpu.VMEM((devices, 1, BLOCK), jnp.float32),
            pltpu.SemaphoreType.DMA((len(CHUNKS),)),
            pltpu.SemaphoreType.DMA,
            pltpu.SemaphoreType.DMA,
            pltpu.SemaphoreType.DMA((sections,)),
            pltpu.SemaphoreType.DMA,
            pltpu.SemaphoreType.DMA,
            pltpu.SemaphoreType.REGULAR,
            pltpu.SemaphoreType.REGULAR,
        ],
        compiler_params=pltpu.CompilerParams(
            collective_id=0, has_side_effects=True, vmem_limit_bytes=32 * 1024 * 1024
        ),
    )(*(in_space(array, pltpu.HBM) for array in (key_weight, value_weight, norm_gain)))
    return pl.pallas_call(
        settle,
        out_shape=(
            jax.ShapeDtypeStruct((sections, share, 2 * ranks * BLOCK), jnp.bfloat16),
            jax.ShapeDtypeStruct(narrow.shape, jnp.float32),
        ),
        in_specs=[in_vmem, in_vmem],
        out_specs=(anywhere, anywhere),
        scratch_shapes=[
            pltpu.SemaphoreType.DMA((sections, 2)),
            pltpu.SemaphoreType.DMA,
        ],
        compiler_params=pltpu.CompilerParams(vmem_limit_bytes=4 * 1024 * 1024),
    )(in_space(wide, pltpu.VMEM), in_space(narrow, pltpu.VMEM))


def solution(mesh):
    placed = (P("section", None, "tensor"), P("section", None, "tensor"), P("section", None))
    return jax.shard_map(
        on_device,
        mesh=mesh,
        in_specs=placed,
        out_specs=(P(None, ("section", "tensor"), None), P(None, "section", None)),
        check_vma=False,
    )
```

```python
import functools
import itertools

import jax
import jax.numpy as jnp
from jax import lax
from jax.experimental import pallas as pl
from jax.experimental.pallas import tpu as pltpu
from jax.sharding import PartitionSpec as P

BLOCK = 128
SCALE_FLOOR = 0.00390625
MESH = pl.DeviceIdType.MESH
SIDE = 4
CHUNK = 4
AHEAD = 3


def hops(offset):
    return sum(min(value, SIDE - value) for value in offset[:3])


def axes_used(offset):
    return sum(value != 0 for value in offset[:3])


def send_order():
    chips = list(itertools.product(range(SIDE), repeat=3))
    kind = {chip: tuple(sorted(min(v, SIDE - v) for v in chip)) for chip in chips}
    order = []
    for alike in sorted(set(kind.values()), key=lambda k: (-sum(k), k)):
        turn = []
        for chip in chips:
            if kind[chip] != alike:
                continue
            for shift in range(3):
                rolled = chip[-shift:] + chip[:-shift] if shift else chip
                for member in (rolled, tuple(-v % SIDE for v in rolled)):
                    if member not in turn:
                        turn.append(member)
        order += [member + (core,) for core in range(2) for member in turn]
    order.remove((0, 0, 0, 0))
    return order


ORDER = send_order()
LINES = [o for o in ORDER if axes_used(o) <= 1]
PLANES = [o for o in ORDER if axes_used(o) == 2]
REST = [o for o in ORDER if axes_used(o) == 3]


def block_of(offset):
    return offset[:2] + (offset[2] // 2, offset[3])


BLOCKS = list(dict.fromkeys(block_of(o) for o in LINES + PLANES + REST))
CHUNKS = [BLOCKS[i : i + CHUNK] for i in range(0, len(BLOCKS), CHUNK)]
PLACE = {block: (i // CHUNK, i % CHUNK) for i, block in enumerate(BLOCKS)}


def exchange(
    sections, ranks, k_ref, v_ref, g_ref, out_ref, scale_ref,
    raw, gain, scaled, rows_out, rows_in,
    load_sem, gain_sem, send_sem, recv_sem, row_send_sem, row_recv_sem, plane_sem, rest_sem,
):
    devices = sections * ranks
    section, rank = lax.axis_index("section"), lax.axis_index("tensor")
    me = section * ranks + rank
    model_rows = k_ref.shape[1]
    part = model_rows // sections
    share = part // ranks
    blocks = part // BLOCK
    core, my_x = section % 2, section // 2 % SIDE
    my_y, my_z = rank // SIDE * 2 + section // (2 * SIDE), rank % SIDE
    toward = 1 - 2 * (my_z % 2)

    def target(offset):
        x, y = (my_x + offset[0]) % SIDE, (my_y + offset[1]) % SIDE
        z = (my_z + toward * offset[2] + SIDE) % SIDE
        return (y % 2 * SIDE + x) * 2 + (core + offset[3]) % 2, y // 2 * SIDE + z

    def block_at(block):
        there, other = target(block[:2] + (block[2] * 2, block[3]))
        return there, other // 2

    def load(chunk):
        for place, block in enumerate(CHUNKS[chunk]):
            there, inner = block_at(block)
            rows = pl.ds(pl.multiple_of(there * part + inner * BLOCK, BLOCK), BLOCK)
            for kind, ref in enumerate((k_ref, v_ref)):
                pltpu.make_async_copy(
                    ref.at[0, rows], raw.at[chunk, kind, place], load_sem.at[chunk]
                ).start()

    lanes = lax.broadcasted_iota(jnp.int32, (1, BLOCK), 1)

    def compute(chunk):
        if chunk + AHEAD < len(CHUNKS):
            load(chunk + AHEAD)
        pltpu.make_async_copy(raw.at[chunk], raw.at[chunk], load_sem.at[chunk]).wait()
        for place, block in enumerate(CHUNKS[chunk]):
            there, inner = block_at(block)
            start = pl.multiple_of(there * part + inner * BLOCK, BLOCK)
            gain_rows = gain[:, pl.ds(start, BLOCK)].astype(jnp.float32)
            gain_rows = jnp.broadcast_to(gain_rows, (BLOCK, BLOCK)).T
            row_values = rows_out[there]
            for kind in range(2):
                folded = gain_rows * raw[chunk, kind, place].astype(jnp.float32)
                folded = folded.astype(jnp.bfloat16).astype(jnp.float32)
                peak = jnp.max(jnp.abs(folded), axis=(0, 1), keepdims=True)
                peak = jnp.maximum(peak, SCALE_FLOOR)
                scaled[chunk, place, kind] = (folded * (1.0 / peak)).astype(jnp.bfloat16)
                lane = (inner * 2 + kind) * ranks + rank
                row_values = jnp.where(lanes == lane, peak, row_values)
            rows_out[there] = row_values

    columns = pl.ds(pl.multiple_of(rank * BLOCK, BLOCK), BLOCK)

    def piece(offset):
        there, other = target(offset)
        chunk, place = PLACE[block_of(offset)]
        half = pl.multiple_of(other % 2 * share, share)
        return there, other, scaled.at[chunk, place, :, pl.ds(half, share)]

    def send(offset):
        there, other, source = piece(offset)
        pltpu.make_async_remote_copy(
            src_ref=source,
            dst_ref=out_ref.at[section, :, :, columns],
            send_sem=send_sem,
            recv_sem=recv_sem.at[section],
            device_id=(there, other),
            device_id_type=MESH,
        ).start()

    def greet(semaphore):
        for offset in LINES:
            pl.semaphore_signal(
                semaphore, inc=1, device_id=target(offset), device_id_type=MESH
            )

    done = 0

    def send_group(group, done):
        for offset in group:
            while PLACE[block_of(offset)][0] >= done:
                compute(done)
                done += 1
            send(offset)
        return done

    barrier = pltpu.get_barrier_semaphore()
    gain_copy = pltpu.make_async_copy(g_ref, gain, gain_sem)
    gain_copy.start()
    load(0)
    greet(barrier)
    for chunk in range(1, AHEAD):
        load(chunk)
    rows_out[...] = jnp.zeros_like(rows_out)
    gain_copy.wait()
    compute(0)
    done = 1
    pl.semaphore_wait(barrier, len(LINES))
    greet(plane_sem)
    done = send_group(LINES, done)
    pl.semaphore_wait(plane_sem, len(LINES))
    greet(rest_sem)
    done = send_group(PLANES[:36], done)
    while done < len(CHUNKS):
        compute(done)
        done += 1
    pl.semaphore_wait(rest_sem, len(LINES))

    @pl.loop(1, devices)
    def _(step):
        peer = lax.rem(me + step, devices)
        there, other = peer // ranks, peer % ranks
        pltpu.make_async_remote_copy(
            src_ref=rows_out.at[there],
            dst_ref=rows_in.at[me],
            send_sem=row_send_sem,
            recv_sem=row_recv_sem,
            device_id=(there, other),
            device_id_type=MESH,
        ).start()

    send_group(REST + PLANES[36:], done)

    out_ref[section, :, :, columns] = piece((0, 0, 0, 0))[2][...]
    rows_in[me] = rows_out[section]

    some_rows = rows_in.at[pl.ds(0, devices - 1)]
    pltpu.make_async_copy(some_rows, some_rows, row_recv_sem).wait()
    peaks = jnp.max(rows_in[...].reshape(sections, ranks, 1, BLOCK), axis=1)
    width = 2 * ranks
    for block in range(blocks):
        for layer in range(sections):
            scale_ref[layer, block : block + 1, :] = peaks[layer, :, block * width : (block + 1) * width]

    for layer in range(sections):

        @pl.when(layer != section)
        def _():
            whole = out_ref.at[layer]
            pltpu.make_async_copy(whole, whole, recv_sem.at[layer]).wait()

        @pl.when(layer == section)
        def _():
            most = out_ref.at[layer, :, :, pl.ds(0, (ranks - 1) * BLOCK)]
            pltpu.make_async_copy(most, most, recv_sem.at[layer]).wait()

    pltpu.make_async_copy(some_rows, some_rows, row_send_sem).wait()
    half = scaled.at[0, 0, :, pl.ds(0, share)]
    all_but_one = scaled.at[pl.ds(0, len(CHUNKS) - 1)]
    pltpu.make_async_copy(all_but_one, all_but_one, send_sem).wait()
    last = scaled.at[0, pl.ds(0, CHUNK - 1)]
    pltpu.make_async_copy(last, last, send_sem).wait()
    pltpu.make_async_copy(half, half, send_sem).wait()


def settle(wide_ref, narrow_ref, scaled_ref, scale_ref, sem, scale_sem):
    layers, kinds, _, columns = wide_ref.shape
    copies = [
        pltpu.make_async_copy(
            wide_ref.at[layer, kind],
            scaled_ref.at[layer, :, pl.ds(kind * columns, columns)],
            sem.at[layer, kind],
        )
        for layer in range(layers)
        for kind in range(kinds)
    ]
    copies.append(pltpu.make_async_copy(narrow_ref, scale_ref, scale_sem))
    for copy in copies:
        copy.start()
    for copy in copies:
        copy.wait()


def on_device(key_weight, value_weight, norm_gain):
    sections, ranks = lax.axis_size("section"), lax.axis_size("tensor")
    devices = sections * ranks
    model_rows = key_weight.shape[1]
    share = model_rows // devices
    blocks = model_rows // sections // BLOCK
    anywhere = pl.BlockSpec(memory_space=pl.ANY)
    in_vmem = pl.BlockSpec(memory_space=pltpu.VMEM)
    in_space = pltpu.with_memory_space_constraint
    wide, narrow = pl.pallas_call(
        functools.partial(exchange, sections, ranks),
        out_shape=(
            pltpu.VMEM((sections, 2, share, ranks * BLOCK), jnp.bfloat16),
            pltpu.VMEM((sections, blocks, 2 * ranks), jnp.float32),
        ),
        in_specs=[anywhere] * 3,
        out_specs=(in_vmem, in_vmem),
        scratch_shapes=[
            pltpu.VMEM((len(CHUNKS), 2, CHUNK, BLOCK, BLOCK), jnp.bfloat16),
            pltpu.VMEM((1, model_rows), jnp.bfloat16),
            pltpu.VMEM((len(CHUNKS), CHUNK, 2, BLOCK, BLOCK), jnp.bfloat16),
            pltpu.VMEM((sections, 1, BLOCK), jnp.float32),
            pltpu.VMEM((devices, 1, BLOCK), jnp.float32),
            pltpu.SemaphoreType.DMA((len(CHUNKS),)),
            pltpu.SemaphoreType.DMA,
            pltpu.SemaphoreType.DMA,
            pltpu.SemaphoreType.DMA((sections,)),
            pltpu.SemaphoreType.DMA,
            pltpu.SemaphoreType.DMA,
            pltpu.SemaphoreType.REGULAR,
            pltpu.SemaphoreType.REGULAR,
        ],
        compiler_params=pltpu.CompilerParams(
            collective_id=0, has_side_effects=True, vmem_limit_bytes=32 * 1024 * 1024
        ),
    )(*(in_space(array, pltpu.HBM) for array in (key_weight, value_weight, norm_gain)))
    return pl.pallas_call(
        settle,
        out_shape=(
            jax.ShapeDtypeStruct((sections, share, 2 * ranks * BLOCK), jnp.bfloat16),
            jax.ShapeDtypeStruct(narrow.shape, jnp.float32),
        ),
        in_specs=[in_vmem, in_vmem],
        out_specs=(anywhere, anywhere),
        scratch_shapes=[
            pltpu.SemaphoreType.DMA((sections, 2)),
            pltpu.SemaphoreType.DMA,
        ],
        compiler_params=pltpu.CompilerParams(vmem_limit_bytes=4 * 1024 * 1024),
    )(in_space(wide, pltpu.VMEM), in_space(narrow, pltpu.VMEM))


def solution(mesh):
    placed = (P("section", None, "tensor"), P("section", None, "tensor"), P("section", None))
    return jax.shard_map(
        on_device,
        mesh=mesh,
        in_specs=placed,
        out_specs=(P(None, ("section", "tensor"), None), P(None, "section", None)),
        check_vma=False,
    )
```

```python
import functools
import itertools

import jax
import jax.numpy as jnp
from jax import lax
from jax.experimental import pallas as pl
from jax.experimental.pallas import tpu as pltpu
from jax.sharding import PartitionSpec as P

BLOCK = 128
SCALE_FLOOR = 0.00390625
MESH = pl.DeviceIdType.MESH
SIDE = 4
CHUNK = 4
AHEAD = 3


def hops(offset):
    return sum(min(value, SIDE - value) for value in offset[:3])


def axes_used(offset):
    return sum(value != 0 for value in offset[:3])


def send_order():
    chips = list(itertools.product(range(SIDE), repeat=3))
    kind = {chip: tuple(sorted(min(v, SIDE - v) for v in chip)) for chip in chips}
    order = []
    for alike in sorted(set(kind.values()), key=lambda k: (-sum(k), k)):
        turn = []
        for chip in chips:
            if kind[chip] != alike:
                continue
            for shift in range(3):
                rolled = chip[-shift:] + chip[:-shift] if shift else chip
                for member in (rolled, tuple(-v % SIDE for v in rolled)):
                    if member not in turn:
                        turn.append(member)
        order += [member + (core,) for core in range(2) for member in turn]
    order.remove((0, 0, 0, 0))
    return order


ORDER = send_order()
LINES = [o for o in ORDER if axes_used(o) <= 1]
PLANES = [o for o in ORDER if axes_used(o) == 2]
REST = [o for o in ORDER if axes_used(o) == 3]


def block_of(offset):
    return offset[:2] + (offset[2] // 2, offset[3])


BLOCKS = list(dict.fromkeys(block_of(o) for o in LINES + PLANES + REST))
CHUNKS = [BLOCKS[i : i + CHUNK] for i in range(0, len(BLOCKS), CHUNK)]
PLACE = {block: (i // CHUNK, i % CHUNK) for i, block in enumerate(BLOCKS)}


def exchange(
    sections, ranks, k_ref, v_ref, g_ref, out_ref, scale_ref,
    raw, gain, scaled, rows_out, rows_in,
    load_sem, gain_sem, send_sem, recv_sem, row_send_sem, row_recv_sem, plane_sem, rest_sem,
):
    devices = sections * ranks
    section, rank = lax.axis_index("section"), lax.axis_index("tensor")
    me = section * ranks + rank
    model_rows = k_ref.shape[1]
    part = model_rows // sections
    share = part // ranks
    blocks = part // BLOCK
    core, my_x = section % 2, section // 2 % SIDE
    my_y, my_z = rank // SIDE * 2 + section // (2 * SIDE), rank % SIDE
    toward = 1 - 2 * (my_z % 2)

    def target(offset):
        x, y = (my_x + offset[0]) % SIDE, (my_y + offset[1]) % SIDE
        z = (my_z + toward * offset[2] + SIDE) % SIDE
        return (y % 2 * SIDE + x) * 2 + (core + offset[3]) % 2, y // 2 * SIDE + z

    def block_at(block):
        there, other = target(block[:2] + (block[2] * 2, block[3]))
        return there, other // 2

    def load(chunk):
        for place, block in enumerate(CHUNKS[chunk]):
            there, inner = block_at(block)
            rows = pl.ds(pl.multiple_of(there * part + inner * BLOCK, BLOCK), BLOCK)
            for kind, ref in enumerate((k_ref, v_ref)):
                pltpu.make_async_copy(
                    ref.at[0, rows], raw.at[(chunk * 2 + kind) * CHUNK + place], load_sem.at[chunk]
                ).start()

    lanes = lax.broadcasted_iota(jnp.int32, (1, BLOCK), 1)

    def compute(chunk):
        if chunk + AHEAD < len(CHUNKS):
            load(chunk + AHEAD)
        here = raw.at[pl.ds(chunk * 2 * CHUNK, 2 * CHUNK)]
        pltpu.make_async_copy(here, here, load_sem.at[chunk]).wait()
        for place, block in enumerate(CHUNKS[chunk]):
            there, inner = block_at(block)
            start = pl.multiple_of(there * part + inner * BLOCK, BLOCK)
            gain_rows = gain[:, pl.ds(start, BLOCK)].astype(jnp.float32)
            gain_rows = jnp.broadcast_to(gain_rows, (BLOCK, BLOCK)).T
            row_values = rows_out[there]
            for kind in range(2):
                folded = gain_rows * raw[(chunk * 2 + kind) * CHUNK + place].astype(jnp.float32)
                folded = folded.astype(jnp.bfloat16).astype(jnp.float32)
                peak = jnp.max(jnp.abs(folded), axis=(0, 1), keepdims=True)
                peak = jnp.maximum(peak, SCALE_FLOOR)
                scaled[chunk, place, kind] = (folded * (1.0 / peak)).astype(jnp.bfloat16)
                lane = (inner * 2 + kind) * ranks + rank
                row_values = jnp.where(lanes == lane, peak, row_values)
            rows_out[there] = row_values

    columns = pl.ds(pl.multiple_of(rank * BLOCK, BLOCK), BLOCK)

    def piece(offset):
        there, other = target(offset)
        chunk, place = PLACE[block_of(offset)]
        half = pl.multiple_of(other % 2 * share, share)
        return there, other, scaled.at[chunk, place, :, pl.ds(half, share)]

    def send(offset):
        there, other, source = piece(offset)
        pltpu.make_async_remote_copy(
            src_ref=source,
            dst_ref=out_ref.at[section, :, :, columns],
            send_sem=send_sem,
            recv_sem=recv_sem,
            device_id=(there, other),
            device_id_type=MESH,
        ).start()

    def greet(semaphore):
        for offset in LINES:
            pl.semaphore_signal(
                semaphore, inc=1, device_id=target(offset), device_id_type=MESH
            )

    done = 0

    def send_group(group, done):
        for offset in group:
            while PLACE[block_of(offset)][0] >= done:
                compute(done)
                done += 1
            send(offset)
        return done

    barrier = pltpu.get_barrier_semaphore()
    gain_copy = pltpu.make_async_copy(g_ref, gain, gain_sem)
    gain_copy.start()
    load(0)
    greet(barrier)
    for chunk in range(1, AHEAD):
        load(chunk)
    rows_out[...] = jnp.zeros_like(rows_out)
    gain_copy.wait()
    compute(0)
    compute(1)
    done = 2
    pl.semaphore_wait(barrier, len(LINES))
    greet(plane_sem)
    done = send_group(LINES, done)
    pl.semaphore_wait(plane_sem, len(LINES))
    greet(rest_sem)
    done = send_group(PLANES[:36], done)
    while done < len(CHUNKS):
        compute(done)
        done += 1
    pl.semaphore_wait(rest_sem, len(LINES))

    @pl.loop(1, devices)
    def _(step):
        peer = lax.rem(me + step, devices)
        there, other = peer // ranks, peer % ranks
        pltpu.make_async_remote_copy(
            src_ref=rows_out.at[there],
            dst_ref=rows_in.at[me],
            send_sem=row_send_sem,
            recv_sem=row_recv_sem,
            device_id=(there, other),
            device_id_type=MESH,
        ).start()

    send_group(REST + PLANES[36:], done)

    out_ref[section, :, :, columns] = piece((0, 0, 0, 0))[2][...]
    rows_in[me] = rows_out[section]

    some_rows = rows_in.at[pl.ds(0, devices - 1)]
    pltpu.make_async_copy(some_rows, some_rows, row_recv_sem).wait()
    peaks = jnp.max(rows_in[...].reshape(sections, ranks, 1, BLOCK), axis=1)
    width = 2 * ranks
    for block in range(blocks):
        for layer in range(sections):
            scale_ref[layer, block : block + 1, :] = peaks[layer, :, block * width : (block + 1) * width]

    pieces = raw.at[pl.ds(0, devices - 1)]
    pltpu.make_async_copy(pieces, pieces, recv_sem).wait()
    pltpu.make_async_copy(some_rows, some_rows, row_send_sem).wait()
    pltpu.make_async_copy(pieces, pieces, send_sem).wait()


def settle(wide_ref, narrow_ref, scaled_ref, scale_ref, sem, scale_sem):
    layers, kinds, _, columns = wide_ref.shape
    copies = [
        pltpu.make_async_copy(
            wide_ref.at[layer, kind],
            scaled_ref.at[layer, :, pl.ds(kind * columns, columns)],
            sem.at[layer, kind],
        )
        for layer in range(layers)
        for kind in range(kinds)
    ]
    copies.append(pltpu.make_async_copy(narrow_ref, scale_ref, scale_sem))
    for copy in copies:
        copy.start()
    for copy in copies:
        copy.wait()


def on_device(key_weight, value_weight, norm_gain):
    sections, ranks = lax.axis_size("section"), lax.axis_size("tensor")
    devices = sections * ranks
    model_rows = key_weight.shape[1]
    share = model_rows // devices
    blocks = model_rows // sections // BLOCK
    anywhere = pl.BlockSpec(memory_space=pl.ANY)
    in_vmem = pl.BlockSpec(memory_space=pltpu.VMEM)
    in_space = pltpu.with_memory_space_constraint
    wide, narrow = pl.pallas_call(
        functools.partial(exchange, sections, ranks),
        out_shape=(
            pltpu.VMEM((sections, 2, share, ranks * BLOCK), jnp.bfloat16),
            pltpu.VMEM((sections, blocks, 2 * ranks), jnp.float32),
        ),
        in_specs=[anywhere] * 3,
        out_specs=(in_vmem, in_vmem),
        scratch_shapes=[
            pltpu.VMEM((len(BLOCKS) * 2, BLOCK, BLOCK), jnp.bfloat16),
            pltpu.VMEM((1, model_rows), jnp.bfloat16),
            pltpu.VMEM((len(CHUNKS), CHUNK, 2, BLOCK, BLOCK), jnp.bfloat16),
            pltpu.VMEM((sections, 1, BLOCK), jnp.float32),
            pltpu.VMEM((devices, 1, BLOCK), jnp.float32),
            pltpu.SemaphoreType.DMA((len(CHUNKS),)),
            pltpu.SemaphoreType.DMA,
            pltpu.SemaphoreType.DMA,
            pltpu.SemaphoreType.DMA,
            pltpu.SemaphoreType.DMA,
            pltpu.SemaphoreType.DMA,
            pltpu.SemaphoreType.REGULAR,
            pltpu.SemaphoreType.REGULAR,
        ],
        compiler_params=pltpu.CompilerParams(
            collective_id=0, has_side_effects=True, vmem_limit_bytes=32 * 1024 * 1024
        ),
    )(*(in_space(array, pltpu.HBM) for array in (key_weight, value_weight, norm_gain)))
    return pl.pallas_call(
        settle,
        out_shape=(
            jax.ShapeDtypeStruct((sections, share, 2 * ranks * BLOCK), jnp.bfloat16),
            jax.ShapeDtypeStruct(narrow.shape, jnp.float32),
        ),
        in_specs=[in_vmem, in_vmem],
        out_specs=(anywhere, anywhere),
        scratch_shapes=[
            pltpu.SemaphoreType.DMA((sections, 2)),
            pltpu.SemaphoreType.DMA,
        ],
        compiler_params=pltpu.CompilerParams(vmem_limit_bytes=4 * 1024 * 1024),
    )(in_space(wide, pltpu.VMEM), in_space(narrow, pltpu.VMEM))


def solution(mesh):
    placed = (P("section", None, "tensor"), P("section", None, "tensor"), P("section", None))
    return jax.shard_map(
        on_device,
        mesh=mesh,
        in_specs=placed,
        out_specs=(P(None, ("section", "tensor"), None), P(None, "section", None)),
        check_vma=False,
    )
```

```python
import functools
import itertools

import jax
import jax.numpy as jnp
from jax import lax
from jax.experimental import pallas as pl
from jax.experimental.pallas import tpu as pltpu
from jax.sharding import PartitionSpec as P

BLOCK = 128
SCALE_FLOOR = 0.00390625
MESH = pl.DeviceIdType.MESH
SIDE = 4
CHUNK = 4
AHEAD = 3


def hops(offset):
    return sum(min(value, SIDE - value) for value in offset[:3])


def axes_used(offset):
    return sum(value != 0 for value in offset[:3])


def send_order():
    chips = list(itertools.product(range(SIDE), repeat=3))
    kind = {chip: tuple(sorted(min(v, SIDE - v) for v in chip)) for chip in chips}
    order = []
    for alike in sorted(set(kind.values()), key=lambda k: (-sum(k), k)):
        turn = []
        for chip in chips:
            if kind[chip] != alike:
                continue
            for shift in range(3):
                rolled = chip[-shift:] + chip[:-shift] if shift else chip
                for member in (rolled, tuple(-v % SIDE for v in rolled)):
                    if member not in turn:
                        turn.append(member)
        order += [member + (core,) for core in range(2) for member in turn]
    order.remove((0, 0, 0, 0))
    return order


ORDER = send_order()
LINES = [o for o in ORDER if axes_used(o) <= 1]
PLANES = [o for o in ORDER if axes_used(o) == 2]
REST = [o for o in ORDER if axes_used(o) == 3]


def block_of(offset):
    return offset[:2] + (offset[2] // 2, offset[3])


BLOCKS = list(dict.fromkeys(block_of(o) for o in LINES + PLANES + REST))
CHUNKS = [BLOCKS[i : i + CHUNK] for i in range(0, len(BLOCKS), CHUNK)]
PLACE = {block: (i // CHUNK, i % CHUNK) for i, block in enumerate(BLOCKS)}


def exchange(
    sections, ranks, k_ref, v_ref, g_ref, out_ref, scale_ref,
    raw, gain, scaled, rows_out, rows_in, rows_at,
    load_sem, gain_sem, send_sem, recv_sem, row_send_sem, row_recv_sem, plane_sem, rest_sem,
):
    devices = sections * ranks
    section, rank = lax.axis_index("section"), lax.axis_index("tensor")
    me = section * ranks + rank
    model_rows = k_ref.shape[1]
    part = model_rows // sections
    share = part // ranks
    blocks = part // BLOCK
    core, my_x = section % 2, section // 2 % SIDE
    my_y, my_z = rank // SIDE * 2 + section // (2 * SIDE), rank % SIDE
    toward = 1 - 2 * (my_z % 2)

    def target(offset):
        x, y = (my_x + offset[0]) % SIDE, (my_y + offset[1]) % SIDE
        z = (my_z + toward * offset[2] + SIDE) % SIDE
        return (y % 2 * SIDE + x) * 2 + (core + offset[3]) % 2, y // 2 * SIDE + z

    def block_at(block):
        there, other = target(block[:2] + (block[2] * 2, block[3]))
        return there, other // 2

    def load(chunk):
        for place, block in enumerate(CHUNKS[chunk]):
            there, inner = block_at(block)
            rows = pl.ds(pl.multiple_of(there * part + inner * BLOCK, BLOCK), BLOCK)
            for kind, ref in enumerate((k_ref, v_ref)):
                pltpu.make_async_copy(
                    ref.at[0, rows], raw.at[(chunk * 2 + kind) * CHUNK + place], load_sem.at[chunk]
                ).start()

    lanes = lax.broadcasted_iota(jnp.int32, (1, BLOCK), 1)

    def compute(chunk):
        if chunk + AHEAD < len(CHUNKS):
            load(chunk + AHEAD)
        here = raw.at[pl.ds(chunk * 2 * CHUNK, 2 * CHUNK)]
        pltpu.make_async_copy(here, here, load_sem.at[chunk]).wait()
        for place, block in enumerate(CHUNKS[chunk]):
            there, inner = block_at(block)
            start = pl.multiple_of(there * part + inner * BLOCK, BLOCK)
            gain_rows = gain[:, pl.ds(start, BLOCK)].astype(jnp.float32)
            gain_rows = jnp.broadcast_to(gain_rows, (BLOCK, BLOCK)).T
            row_values = rows_out[there]
            for kind in range(2):
                folded = gain_rows * raw[(chunk * 2 + kind) * CHUNK + place].astype(jnp.float32)
                folded = folded.astype(jnp.bfloat16).astype(jnp.float32)
                peak = jnp.max(jnp.abs(folded), axis=(0, 1), keepdims=True)
                peak = jnp.maximum(peak, SCALE_FLOOR)
                scaled[chunk, place, kind] = (folded * (1.0 / peak)).astype(jnp.bfloat16)
                lane = (kind * sections + section) * blocks + inner
                row_values = jnp.where(lanes == lane, peak, row_values)
            rows_out[there] = row_values

    columns = pl.ds(pl.multiple_of(rank * BLOCK, BLOCK), BLOCK)

    def piece(offset):
        there, other = target(offset)
        chunk, place = PLACE[block_of(offset)]
        half = pl.multiple_of(other % 2 * share, share)
        return there, other, scaled.at[chunk, place, :, pl.ds(half, share)]

    def send(offset):
        there, other, source = piece(offset)
        pltpu.make_async_remote_copy(
            src_ref=source,
            dst_ref=out_ref.at[section, :, :, columns],
            send_sem=send_sem,
            recv_sem=recv_sem,
            device_id=(there, other),
            device_id_type=MESH,
        ).start()

    def greet(semaphore):
        for offset in LINES:
            pl.semaphore_signal(
                semaphore, inc=1, device_id=target(offset), device_id_type=MESH
            )

    done = 0

    def send_group(group, done):
        for offset in group:
            while PLACE[block_of(offset)][0] >= done:
                compute(done)
                done += 1
            send(offset)
        return done

    barrier = pltpu.get_barrier_semaphore()
    gain_copy = pltpu.make_async_copy(g_ref, gain, gain_sem)
    gain_copy.start()
    load(0)
    greet(barrier)
    for chunk in range(1, AHEAD):
        load(chunk)
    rows_out[...] = jnp.zeros_like(rows_out)
    gain_copy.wait()
    compute(0)
    compute(1)
    done = 2
    pl.semaphore_wait(barrier, len(LINES))
    greet(plane_sem)
    done = send_group(LINES, done)
    pl.semaphore_wait(plane_sem, len(LINES))
    greet(rest_sem)
    done = send_group(PLANES[:36], done)
    while done < len(CHUNKS):
        compute(done)
        done += 1
    pl.semaphore_wait(rest_sem, len(LINES))

    def send_row(source, landing, there, other, stage):
        pltpu.make_async_remote_copy(
            src_ref=source,
            dst_ref=landing,
            send_sem=row_send_sem.at[stage],
            recv_sem=row_recv_sem.at[stage],
            device_id=(there, other),
            device_id_type=MESH,
        ).start()

    def wait_rows(semaphores, stage, count):
        some = rows_in.at[pl.ds(0, count)]
        pltpu.make_async_copy(some, some, semaphores.at[stage]).wait()

    @pl.loop(1, sections)
    def _(step):
        there = lax.rem(section + step, sections)
        send_row(rows_out.at[there], rows_in.at[section], there, rank, 0)

    send_group(REST + PLANES[36:], done)
    rows_in[section] = rows_out[section]
    wait_rows(row_recv_sem, 0, sections - 1)
    rows_at[rank] = jnp.max(rows_in[...], axis=0)
    out_ref[section, :, :, columns] = piece((0, 0, 0, 0))[2][...]

    @pl.loop(1, ranks)
    def _(step):
        other = lax.rem(rank + step, ranks)
        send_row(rows_at.at[rank], rows_at.at[rank], section, other, 1)

    wait_rows(row_recv_sem, 1, ranks - 1)
    by_rank = jnp.concatenate([rows_at[other] for other in range(ranks)] * (BLOCK // ranks), axis=0).T
    first_half, second_half = by_rank[: BLOCK // 2], by_rank[BLOCK // 2 :]
    all_scales = jnp.where(lanes < ranks, first_half, second_half)
    for layer in range(sections):
        scale_ref[layer] = all_scales[layer * blocks : (layer + 1) * blocks, : 2 * ranks]

    pieces = raw.at[pl.ds(0, devices - 1)]
    pltpu.make_async_copy(pieces, pieces, recv_sem).wait()
    wait_rows(row_send_sem, 0, sections - 1)
    wait_rows(row_send_sem, 1, ranks - 1)
    pltpu.make_async_copy(pieces, pieces, send_sem).wait()


def settle(wide_ref, narrow_ref, scaled_ref, scale_ref, sem, scale_sem):
    layers, kinds, _, columns = wide_ref.shape
    copies = [
        pltpu.make_async_copy(
            wide_ref.at[layer, kind],
            scaled_ref.at[layer, :, pl.ds(kind * columns, columns)],
            sem.at[layer, kind],
        )
        for layer in range(layers)
        for kind in range(kinds)
    ]
    copies.append(pltpu.make_async_copy(narrow_ref, scale_ref, scale_sem))
    for copy in copies:
        copy.start()
    for copy in copies:
        copy.wait()


def on_device(key_weight, value_weight, norm_gain):
    sections, ranks = lax.axis_size("section"), lax.axis_size("tensor")
    devices = sections * ranks
    model_rows = key_weight.shape[1]
    share = model_rows // devices
    blocks = model_rows // sections // BLOCK
    anywhere = pl.BlockSpec(memory_space=pl.ANY)
    in_vmem = pl.BlockSpec(memory_space=pltpu.VMEM)
    in_space = pltpu.with_memory_space_constraint
    wide, narrow = pl.pallas_call(
        functools.partial(exchange, sections, ranks),
        out_shape=(
            pltpu.VMEM((sections, 2, share, ranks * BLOCK), jnp.bfloat16),
            pltpu.VMEM((sections, blocks, 2 * ranks), jnp.float32),
        ),
        in_specs=[anywhere] * 3,
        out_specs=(in_vmem, in_vmem),
        scratch_shapes=[
            pltpu.VMEM((len(BLOCKS) * 2, BLOCK, BLOCK), jnp.bfloat16),
            pltpu.VMEM((1, model_rows), jnp.bfloat16),
            pltpu.VMEM((len(CHUNKS), CHUNK, 2, BLOCK, BLOCK), jnp.bfloat16),
            pltpu.VMEM((sections, 1, BLOCK), jnp.float32),
            pltpu.VMEM((sections, 1, BLOCK), jnp.float32),
            pltpu.VMEM((ranks, 1, BLOCK), jnp.float32),
            pltpu.SemaphoreType.DMA((len(CHUNKS),)),
            pltpu.SemaphoreType.DMA,
            pltpu.SemaphoreType.DMA,
            pltpu.SemaphoreType.DMA,
            pltpu.SemaphoreType.DMA((2,)),
            pltpu.SemaphoreType.DMA((2,)),
            pltpu.SemaphoreType.REGULAR,
            pltpu.SemaphoreType.REGULAR,
        ],
        compiler_params=pltpu.CompilerParams(
            collective_id=0, has_side_effects=True, vmem_limit_bytes=32 * 1024 * 1024
        ),
    )(*(in_space(array, pltpu.HBM) for array in (key_weight, value_weight, norm_gain)))
    return pl.pallas_call(
        settle,
        out_shape=(
            jax.ShapeDtypeStruct((sections, share, 2 * ranks * BLOCK), jnp.bfloat16),
            jax.ShapeDtypeStruct(narrow.shape, jnp.float32),
        ),
        in_specs=[in_vmem, in_vmem],
        out_specs=(anywhere, anywhere),
        scratch_shapes=[
            pltpu.SemaphoreType.DMA((sections, 2)),
            pltpu.SemaphoreType.DMA,
        ],
        compiler_params=pltpu.CompilerParams(vmem_limit_bytes=4 * 1024 * 1024),
    )(in_space(wide, pltpu.VMEM), in_space(narrow, pltpu.VMEM))


def solution(mesh):
    placed = (P("section", None, "tensor"), P("section", None, "tensor"), P("section", None))
    return jax.shard_map(
        on_device,
        mesh=mesh,
        in_specs=placed,
        out_specs=(P(None, ("section", "tensor"), None), P(None, "section", None)),
        check_vma=False,
    )
```

```python
import functools
import itertools

import jax
import jax.numpy as jnp
from jax import lax
from jax.experimental import pallas as pl
from jax.experimental.pallas import tpu as pltpu
from jax.sharding import PartitionSpec as P

BLOCK = 128
SCALE_FLOOR = 0.00390625
MESH = pl.DeviceIdType.MESH
SIDE = 4
CHUNK = 4
AHEAD = 3


def hops(offset):
    return sum(min(value, SIDE - value) for value in offset[:3])


def axes_used(offset):
    return sum(value != 0 for value in offset[:3])


def send_order():
    chips = list(itertools.product(range(SIDE), repeat=3))
    kind = {chip: tuple(sorted(min(v, SIDE - v) for v in chip)) for chip in chips}
    order = []
    for alike in sorted(set(kind.values()), key=lambda k: (-sum(k), k)):
        turn = []
        for chip in chips:
            if kind[chip] != alike:
                continue
            for shift in range(3):
                rolled = chip[-shift:] + chip[:-shift] if shift else chip
                for member in (rolled, tuple(-v % SIDE for v in rolled)):
                    if member not in turn:
                        turn.append(member)
        order += [member + (core,) for core in range(2) for member in turn]
    order.remove((0, 0, 0, 0))
    return order


ORDER = send_order()
LINES = [o for o in ORDER if axes_used(o) <= 1]
SAME_CORE = [o for o in LINES if o[3] == 0]
PLANES = [o for o in ORDER if axes_used(o) == 2]
REST = [o for o in ORDER if axes_used(o) == 3]


def block_of(offset):
    return offset[:2] + (offset[2] // 2, offset[3])


BLOCKS = list(dict.fromkeys(block_of(o) for o in LINES + PLANES + REST))
CHUNKS = [BLOCKS[i : i + CHUNK] for i in range(0, len(BLOCKS), CHUNK)]
PLACE = {block: (i // CHUNK, i % CHUNK) for i, block in enumerate(BLOCKS)}


def exchange(
    sections, ranks, k_ref, v_ref, g_ref, out_ref, scale_ref,
    raw, gain, scaled, rows_out, rows_in, rows_at,
    load_sem, gain_sem, send_sem, recv_sem, row_send_sem, row_recv_sem, plane_sem, rest_sem,
):
    devices = sections * ranks
    section, rank = lax.axis_index("section"), lax.axis_index("tensor")
    me = section * ranks + rank
    model_rows = k_ref.shape[1]
    part = model_rows // sections
    share = part // ranks
    blocks = part // BLOCK
    core, my_x = section % 2, section // 2 % SIDE
    my_y, my_z = rank // SIDE * 2 + section // (2 * SIDE), rank % SIDE
    toward = 1 - 2 * (my_z % 2)

    def target(offset):
        x, y = (my_x + offset[0]) % SIDE, (my_y + offset[1]) % SIDE
        z = (my_z + toward * offset[2] + SIDE) % SIDE
        return (y % 2 * SIDE + x) * 2 + (core + offset[3]) % 2, y // 2 * SIDE + z

    def block_at(block):
        there, other = target(block[:2] + (block[2] * 2, block[3]))
        return there, other // 2

    def load(chunk):
        for place, block in enumerate(CHUNKS[chunk]):
            there, inner = block_at(block)
            rows = pl.ds(pl.multiple_of(there * part + inner * BLOCK, BLOCK), BLOCK)
            for kind, ref in enumerate((k_ref, v_ref)):
                pltpu.make_async_copy(
                    ref.at[0, rows], raw.at[(chunk * 2 + kind) * CHUNK + place], load_sem.at[chunk]
                ).start()

    lanes = lax.broadcasted_iota(jnp.int32, (1, BLOCK), 1)

    def compute(chunk):
        if chunk + AHEAD < len(CHUNKS):
            load(chunk + AHEAD)
        here = raw.at[pl.ds(chunk * 2 * CHUNK, 2 * CHUNK)]
        pltpu.make_async_copy(here, here, load_sem.at[chunk]).wait()
        for place, block in enumerate(CHUNKS[chunk]):
            there, inner = block_at(block)
            start = pl.multiple_of(there * part + inner * BLOCK, BLOCK)
            gain_rows = gain[:, pl.ds(start, BLOCK)].astype(jnp.float32)
            gain_rows = jnp.broadcast_to(gain_rows, (BLOCK, BLOCK)).T
            row_values = rows_out[there]
            for kind in range(2):
                folded = gain_rows * raw[(chunk * 2 + kind) * CHUNK + place].astype(jnp.float32)
                folded = folded.astype(jnp.bfloat16).astype(jnp.float32)
                peak = jnp.max(jnp.abs(folded), axis=(0, 1), keepdims=True)
                peak = jnp.maximum(peak, SCALE_FLOOR)
                scaled[chunk, place, kind] = (folded * (1.0 / peak)).astype(jnp.bfloat16)
                lane = (kind * sections + section) * blocks + inner
                row_values = jnp.where(lanes == lane, peak, row_values)
            rows_out[there] = row_values

    columns = pl.ds(pl.multiple_of(rank * BLOCK, BLOCK), BLOCK)

    def piece(offset):
        there, other = target(offset)
        chunk, place = PLACE[block_of(offset)]
        half = pl.multiple_of(other % 2 * share, share)
        return there, other, scaled.at[chunk, place, :, pl.ds(half, share)]

    def send(offset):
        there, other, source = piece(offset)
        pltpu.make_async_remote_copy(
            src_ref=source,
            dst_ref=out_ref.at[section, :, :, columns],
            send_sem=send_sem,
            recv_sem=recv_sem,
            device_id=(there, other),
            device_id_type=MESH,
        ).start()

    def greet(semaphore, peers):
        for offset in peers:
            pl.semaphore_signal(
                semaphore, inc=1, device_id=target(offset), device_id_type=MESH
            )

    done = 0

    def send_group(group, done):
        for offset in group:
            while PLACE[block_of(offset)][0] >= done:
                compute(done)
                done += 1
            send(offset)
        return done

    barrier = pltpu.get_barrier_semaphore()
    gain_copy = pltpu.make_async_copy(g_ref, gain, gain_sem)
    gain_copy.start()
    load(0)
    greet(barrier, LINES)
    for chunk in range(1, AHEAD):
        load(chunk)
    rows_out[...] = jnp.zeros_like(rows_out)
    gain_copy.wait()
    compute(0)
    compute(1)
    done = 2
    pl.semaphore_wait(barrier, len(LINES))
    greet(plane_sem, SAME_CORE)
    done = send_group(LINES, done)
    pl.semaphore_wait(plane_sem, len(SAME_CORE))
    greet(rest_sem, SAME_CORE)
    done = send_group(PLANES[:36], done)
    while done < len(CHUNKS):
        compute(done)
        done += 1
    pl.semaphore_wait(rest_sem, len(SAME_CORE))

    def send_row(source, landing, there, other, stage):
        pltpu.make_async_remote_copy(
            src_ref=source,
            dst_ref=landing,
            send_sem=row_send_sem.at[stage],
            recv_sem=row_recv_sem.at[stage],
            device_id=(there, other),
            device_id_type=MESH,
        ).start()

    def wait_rows(semaphores, stage, count):
        some = rows_in.at[pl.ds(0, count)]
        pltpu.make_async_copy(some, some, semaphores.at[stage]).wait()

    @pl.loop(1, sections)
    def _(step):
        there = lax.rem(section + step, sections)
        send_row(rows_out.at[there], rows_in.at[section], there, rank, 0)

    send_group(REST + PLANES[36:], done)
    rows_in[section] = rows_out[section]
    wait_rows(row_recv_sem, 0, sections - 1)
    rows_at[rank] = jnp.max(rows_in[...], axis=0)
    out_ref[section, :, :, columns] = piece((0, 0, 0, 0))[2][...]

    @pl.loop(1, ranks)
    def _(step):
        other = lax.rem(rank + step, ranks)
        send_row(rows_at.at[rank], rows_at.at[rank], section, other, 1)

    wait_rows(row_recv_sem, 1, ranks - 1)
    by_rank = jnp.concatenate([rows_at[other] for other in range(ranks)] * (BLOCK // ranks), axis=0).T
    first_half, second_half = by_rank[: BLOCK // 2], by_rank[BLOCK // 2 :]
    all_scales = jnp.where(lanes < ranks, first_half, second_half)
    for layer in range(sections):
        scale_ref[layer] = all_scales[layer * blocks : (layer + 1) * blocks, : 2 * ranks]

    pieces = raw.at[pl.ds(0, devices - 1)]
    pltpu.make_async_copy(pieces, pieces, recv_sem).wait()
    wait_rows(row_send_sem, 0, sections - 1)
    wait_rows(row_send_sem, 1, ranks - 1)
    pltpu.make_async_copy(pieces, pieces, send_sem).wait()


def settle(wide_ref, narrow_ref, scaled_ref, scale_ref, sem, scale_sem):
    layers, kinds, _, columns = wide_ref.shape
    copies = [
        pltpu.make_async_copy(
            wide_ref.at[layer, kind],
            scaled_ref.at[layer, :, pl.ds(kind * columns, columns)],
            sem.at[layer, kind],
        )
        for layer in range(layers)
        for kind in range(kinds)
    ]
    copies.append(pltpu.make_async_copy(narrow_ref, scale_ref, scale_sem))
    for copy in copies:
        copy.start()
    for copy in copies:
        copy.wait()


def on_device(key_weight, value_weight, norm_gain):
    sections, ranks = lax.axis_size("section"), lax.axis_size("tensor")
    devices = sections * ranks
    model_rows = key_weight.shape[1]
    share = model_rows // devices
    blocks = model_rows // sections // BLOCK
    anywhere = pl.BlockSpec(memory_space=pl.ANY)
    in_vmem = pl.BlockSpec(memory_space=pltpu.VMEM)
    in_space = pltpu.with_memory_space_constraint
    wide, narrow = pl.pallas_call(
        functools.partial(exchange, sections, ranks),
        out_shape=(
            pltpu.VMEM((sections, 2, share, ranks * BLOCK), jnp.bfloat16),
            pltpu.VMEM((sections, blocks, 2 * ranks), jnp.float32),
        ),
        in_specs=[anywhere] * 3,
        out_specs=(in_vmem, in_vmem),
        scratch_shapes=[
            pltpu.VMEM((len(BLOCKS) * 2, BLOCK, BLOCK), jnp.bfloat16),
            pltpu.VMEM((1, model_rows), jnp.bfloat16),
            pltpu.VMEM((len(CHUNKS), CHUNK, 2, BLOCK, BLOCK), jnp.bfloat16),
            pltpu.VMEM((sections, 1, BLOCK), jnp.float32),
            pltpu.VMEM((sections, 1, BLOCK), jnp.float32),
            pltpu.VMEM((ranks, 1, BLOCK), jnp.float32),
            pltpu.SemaphoreType.DMA((len(CHUNKS),)),
            pltpu.SemaphoreType.DMA,
            pltpu.SemaphoreType.DMA,
            pltpu.SemaphoreType.DMA,
            pltpu.SemaphoreType.DMA((2,)),
            pltpu.SemaphoreType.DMA((2,)),
            pltpu.SemaphoreType.REGULAR,
            pltpu.SemaphoreType.REGULAR,
        ],
        compiler_params=pltpu.CompilerParams(
            collective_id=0, has_side_effects=True, vmem_limit_bytes=32 * 1024 * 1024
        ),
    )(*(in_space(array, pltpu.HBM) for array in (key_weight, value_weight, norm_gain)))
    return pl.pallas_call(
        settle,
        out_shape=(
            jax.ShapeDtypeStruct((sections, share, 2 * ranks * BLOCK), jnp.bfloat16),
            jax.ShapeDtypeStruct(narrow.shape, jnp.float32),
        ),
        in_specs=[in_vmem, in_vmem],
        out_specs=(anywhere, anywhere),
        scratch_shapes=[
            pltpu.SemaphoreType.DMA((sections, 2)),
            pltpu.SemaphoreType.DMA,
        ],
        compiler_params=pltpu.CompilerParams(vmem_limit_bytes=4 * 1024 * 1024),
    )(in_space(wide, pltpu.VMEM), in_space(narrow, pltpu.VMEM))


def solution(mesh):
    placed = (P("section", None, "tensor"), P("section", None, "tensor"), P("section", None))
    return jax.shard_map(
        on_device,
        mesh=mesh,
        in_specs=placed,
        out_specs=(P(None, ("section", "tensor"), None), P(None, "section", None)),
        check_vma=False,
    )
```

```python
import functools
import itertools

import jax
import jax.numpy as jnp
from jax import lax
from jax.experimental import pallas as pl
from jax.experimental.pallas import tpu as pltpu
from jax.sharding import PartitionSpec as P

BLOCK = 128
SCALE_FLOOR = 0.00390625
MESH = pl.DeviceIdType.MESH
SIDE = 4
CHUNK = 4
AHEAD = 3


def hops(offset):
    return sum(min(value, SIDE - value) for value in offset[:3])


def axes_used(offset):
    return sum(value != 0 for value in offset[:3])


def send_order():
    chips = list(itertools.product(range(SIDE), repeat=3))
    kind = {chip: tuple(sorted(min(v, SIDE - v) for v in chip)) for chip in chips}
    order = []
    for alike in sorted(set(kind.values()), key=lambda k: (-sum(k), k)):
        turn = []
        for chip in chips:
            if kind[chip] != alike:
                continue
            for shift in range(3):
                rolled = chip[-shift:] + chip[:-shift] if shift else chip
                for member in (rolled, tuple(-v % SIDE for v in rolled)):
                    if member not in turn:
                        turn.append(member)
        order += [member + (core,) for core in range(2) for member in turn]
    order.remove((0, 0, 0, 0))
    return order


ORDER = send_order()
LINES = [o for o in ORDER if axes_used(o) <= 1]
ALONG_YZ = [o for o in LINES if o[3] == 0 and o[0] == 0]
ALONG_X = [o for o in LINES if o[3] == 0 and o[0] != 0]
PLANES = [o for o in ORDER if axes_used(o) == 2]
REST = [o for o in ORDER if axes_used(o) == 3]


def block_of(offset):
    return offset[:2] + (offset[2] // 2, offset[3])


BLOCKS = list(dict.fromkeys(block_of(o) for o in LINES + PLANES + REST))
CHUNKS = [BLOCKS[i : i + CHUNK] for i in range(0, len(BLOCKS), CHUNK)]
PLACE = {block: (i // CHUNK, i % CHUNK) for i, block in enumerate(BLOCKS)}


def exchange(
    sections, ranks, k_ref, v_ref, g_ref, out_ref, scale_ref,
    raw, gain, scaled, rows_out, rows_in, rows_at,
    load_sem, gain_sem, send_sem, recv_sem, row_send_sem, row_recv_sem, plane_sem, rest_sem,
):
    devices = sections * ranks
    section, rank = lax.axis_index("section"), lax.axis_index("tensor")
    me = section * ranks + rank
    model_rows = k_ref.shape[1]
    part = model_rows // sections
    share = part // ranks
    blocks = part // BLOCK
    core, my_x = section % 2, section // 2 % SIDE
    my_y, my_z = rank // SIDE * 2 + section // (2 * SIDE), rank % SIDE
    toward = 1 - 2 * (my_z % 2)

    def target(offset):
        x, y = (my_x + offset[0]) % SIDE, (my_y + offset[1]) % SIDE
        z = (my_z + toward * offset[2] + SIDE) % SIDE
        return (y % 2 * SIDE + x) * 2 + (core + offset[3]) % 2, y // 2 * SIDE + z

    def block_at(block):
        there, other = target(block[:2] + (block[2] * 2, block[3]))
        return there, other // 2

    def load(chunk):
        for place, block in enumerate(CHUNKS[chunk]):
            there, inner = block_at(block)
            rows = pl.ds(pl.multiple_of(there * part + inner * BLOCK, BLOCK), BLOCK)
            for kind, ref in enumerate((k_ref, v_ref)):
                pltpu.make_async_copy(
                    ref.at[0, rows], raw.at[(chunk * 2 + kind) * CHUNK + place], load_sem.at[chunk]
                ).start()

    lanes = lax.broadcasted_iota(jnp.int32, (1, BLOCK), 1)

    def compute(chunk):
        if chunk + AHEAD < len(CHUNKS):
            load(chunk + AHEAD)
        here = raw.at[pl.ds(chunk * 2 * CHUNK, 2 * CHUNK)]
        pltpu.make_async_copy(here, here, load_sem.at[chunk]).wait()
        for place, block in enumerate(CHUNKS[chunk]):
            there, inner = block_at(block)
            start = pl.multiple_of(there * part + inner * BLOCK, BLOCK)
            gain_rows = gain[:, pl.ds(start, BLOCK)].astype(jnp.float32)
            gain_rows = jnp.broadcast_to(gain_rows, (BLOCK, BLOCK)).T
            row_values = rows_out[there]
            for kind in range(2):
                folded = gain_rows * raw[(chunk * 2 + kind) * CHUNK + place].astype(jnp.float32)
                folded = folded.astype(jnp.bfloat16).astype(jnp.float32)
                peak = jnp.max(jnp.abs(folded), axis=(0, 1), keepdims=True)
                peak = jnp.maximum(peak, SCALE_FLOOR)
                scaled[chunk, place, kind] = (folded * (1.0 / peak)).astype(jnp.bfloat16)
                lane = (kind * sections + section) * blocks + inner
                row_values = jnp.where(lanes == lane, peak, row_values)
            rows_out[there] = row_values

    columns = pl.ds(pl.multiple_of(rank * BLOCK, BLOCK), BLOCK)

    def piece(offset):
        there, other = target(offset)
        chunk, place = PLACE[block_of(offset)]
        half = pl.multiple_of(other % 2 * share, share)
        return there, other, scaled.at[chunk, place, :, pl.ds(half, share)]

    def send(offset):
        there, other, source = piece(offset)
        pltpu.make_async_remote_copy(
            src_ref=source,
            dst_ref=out_ref.at[section, :, :, columns],
            send_sem=send_sem,
            recv_sem=recv_sem,
            device_id=(there, other),
            device_id_type=MESH,
        ).start()

    def greet(semaphore, peers):
        for offset in peers:
            pl.semaphore_signal(
                semaphore, inc=1, device_id=target(offset), device_id_type=MESH
            )

    done = 0

    def send_group(group, done):
        for offset in group:
            while PLACE[block_of(offset)][0] >= done:
                compute(done)
                done += 1
            send(offset)
        return done

    barrier = pltpu.get_barrier_semaphore()
    gain_copy = pltpu.make_async_copy(g_ref, gain, gain_sem)
    gain_copy.start()
    load(0)
    greet(barrier, LINES)
    for chunk in range(1, AHEAD):
        load(chunk)
    rows_out[...] = jnp.zeros_like(rows_out)
    gain_copy.wait()
    compute(0)
    compute(1)
    done = 2
    pl.semaphore_wait(barrier, len(LINES))
    greet(plane_sem, ALONG_YZ)
    done = send_group(LINES, done)
    pl.semaphore_wait(plane_sem, len(ALONG_YZ))
    greet(rest_sem, ALONG_X)
    done = send_group(PLANES[:36], done)
    while done < len(CHUNKS):
        compute(done)
        done += 1
    pl.semaphore_wait(rest_sem, len(ALONG_X))

    def send_row(source, landing, there, other, stage):
        pltpu.make_async_remote_copy(
            src_ref=source,
            dst_ref=landing,
            send_sem=row_send_sem.at[stage],
            recv_sem=row_recv_sem.at[stage],
            device_id=(there, other),
            device_id_type=MESH,
        ).start()

    def wait_rows(semaphores, stage, count):
        some = rows_in.at[pl.ds(0, count)]
        pltpu.make_async_copy(some, some, semaphores.at[stage]).wait()

    @pl.loop(1, sections)
    def _(step):
        there = lax.rem(section + step, sections)
        send_row(rows_out.at[there], rows_in.at[section], there, rank, 0)

    send_group(REST + PLANES[36:], done)
    rows_in[section] = rows_out[section]
    wait_rows(row_recv_sem, 0, sections - 1)
    rows_at[rank] = jnp.max(rows_in[...], axis=0)
    out_ref[section, :, :, columns] = piece((0, 0, 0, 0))[2][...]

    @pl.loop(1, ranks)
    def _(step):
        other = lax.rem(rank + step, ranks)
        send_row(rows_at.at[rank], rows_at.at[rank], section, other, 1)

    wait_rows(row_recv_sem, 1, ranks - 1)
    by_rank = jnp.concatenate([rows_at[other] for other in range(ranks)] * (BLOCK // ranks), axis=0).T
    first_half, second_half = by_rank[: BLOCK // 2], by_rank[BLOCK // 2 :]
    all_scales = jnp.where(lanes < ranks, first_half, second_half)
    for layer in range(sections):
        scale_ref[layer] = all_scales[layer * blocks : (layer + 1) * blocks, : 2 * ranks]

    pieces = raw.at[pl.ds(0, devices - 1)]
    pltpu.make_async_copy(pieces, pieces, recv_sem).wait()
    wait_rows(row_send_sem, 0, sections - 1)
    wait_rows(row_send_sem, 1, ranks - 1)
    pltpu.make_async_copy(pieces, pieces, send_sem).wait()


def settle(wide_ref, narrow_ref, scaled_ref, scale_ref, sem, scale_sem):
    layers, kinds, _, columns = wide_ref.shape
    copies = [
        pltpu.make_async_copy(
            wide_ref.at[layer, kind],
            scaled_ref.at[layer, :, pl.ds(kind * columns, columns)],
            sem.at[layer, kind],
        )
        for layer in range(layers)
        for kind in range(kinds)
    ]
    copies.append(pltpu.make_async_copy(narrow_ref, scale_ref, scale_sem))
    for copy in copies:
        copy.start()
    for copy in copies:
        copy.wait()


def on_device(key_weight, value_weight, norm_gain):
    sections, ranks = lax.axis_size("section"), lax.axis_size("tensor")
    devices = sections * ranks
    model_rows = key_weight.shape[1]
    share = model_rows // devices
    blocks = model_rows // sections // BLOCK
    anywhere = pl.BlockSpec(memory_space=pl.ANY)
    in_vmem = pl.BlockSpec(memory_space=pltpu.VMEM)
    in_space = pltpu.with_memory_space_constraint
    wide, narrow = pl.pallas_call(
        functools.partial(exchange, sections, ranks),
        out_shape=(
            pltpu.VMEM((sections, 2, share, ranks * BLOCK), jnp.bfloat16),
            pltpu.VMEM((sections, blocks, 2 * ranks), jnp.float32),
        ),
        in_specs=[anywhere] * 3,
        out_specs=(in_vmem, in_vmem),
        scratch_shapes=[
            pltpu.VMEM((len(BLOCKS) * 2, BLOCK, BLOCK), jnp.bfloat16),
            pltpu.VMEM((1, model_rows), jnp.bfloat16),
            pltpu.VMEM((len(CHUNKS), CHUNK, 2, BLOCK, BLOCK), jnp.bfloat16),
            pltpu.VMEM((sections, 1, BLOCK), jnp.float32),
            pltpu.VMEM((sections, 1, BLOCK), jnp.float32),
            pltpu.VMEM((ranks, 1, BLOCK), jnp.float32),
            pltpu.SemaphoreType.DMA((len(CHUNKS),)),
            pltpu.SemaphoreType.DMA,
            pltpu.SemaphoreType.DMA,
            pltpu.SemaphoreType.DMA,
            pltpu.SemaphoreType.DMA((2,)),
            pltpu.SemaphoreType.DMA((2,)),
            pltpu.SemaphoreType.REGULAR,
            pltpu.SemaphoreType.REGULAR,
        ],
        compiler_params=pltpu.CompilerParams(
            collective_id=0, has_side_effects=True, vmem_limit_bytes=32 * 1024 * 1024
        ),
    )(*(in_space(array, pltpu.HBM) for array in (key_weight, value_weight, norm_gain)))
    return pl.pallas_call(
        settle,
        out_shape=(
            jax.ShapeDtypeStruct((sections, share, 2 * ranks * BLOCK), jnp.bfloat16),
            jax.ShapeDtypeStruct(narrow.shape, jnp.float32),
        ),
        in_specs=[in_vmem, in_vmem],
        out_specs=(anywhere, anywhere),
        scratch_shapes=[
            pltpu.SemaphoreType.DMA((sections, 2)),
            pltpu.SemaphoreType.DMA,
        ],
        compiler_params=pltpu.CompilerParams(vmem_limit_bytes=4 * 1024 * 1024),
    )(in_space(wide, pltpu.VMEM), in_space(narrow, pltpu.VMEM))


def solution(mesh):
    placed = (P("section", None, "tensor"), P("section", None, "tensor"), P("section", None))
    return jax.shard_map(
        on_device,
        mesh=mesh,
        in_specs=placed,
        out_specs=(P(None, ("section", "tensor"), None), P(None, "section", None)),
        check_vma=False,
    )
```

```python
import functools
import itertools

import jax
import jax.numpy as jnp
from jax import lax
from jax.experimental import pallas as pl
from jax.experimental.pallas import tpu as pltpu
from jax.sharding import PartitionSpec as P

BLOCK = 128
SCALE_FLOOR = 0.00390625
MESH = pl.DeviceIdType.MESH
SIDE = 4
CHUNK = 4
AHEAD = 3


def hops(offset):
    return sum(min(value, SIDE - value) for value in offset[:3])


def axes_used(offset):
    return sum(value != 0 for value in offset[:3])


def send_order():
    chips = list(itertools.product(range(SIDE), repeat=3))
    kind = {chip: tuple(sorted(min(v, SIDE - v) for v in chip)) for chip in chips}
    order = []
    for alike in sorted(set(kind.values()), key=lambda k: (-sum(k), k)):
        turn = []
        for chip in chips:
            if kind[chip] != alike:
                continue
            for shift in range(3):
                rolled = chip[-shift:] + chip[:-shift] if shift else chip
                for member in (rolled, tuple(-v % SIDE for v in rolled)):
                    if member not in turn:
                        turn.append(member)
        order += [member + (core,) for core in range(2) for member in turn]
    order.remove((0, 0, 0, 0))
    return order


ORDER = send_order()
LINES = [o for o in ORDER if axes_used(o) <= 1]
SAME_CORE = [o for o in LINES if o[3] == 0]
ALONG_X = [o for o in SAME_CORE if o[0] != 0]
PLANES = [o for o in ORDER if axes_used(o) == 2]
REST = [o for o in ORDER if axes_used(o) == 3]


def block_of(offset):
    return offset[:2] + (offset[2] // 2, offset[3])


BLOCKS = list(dict.fromkeys(block_of(o) for o in LINES + PLANES + REST))
CHUNKS = [BLOCKS[i : i + CHUNK] for i in range(0, len(BLOCKS), CHUNK)]
PLACE = {block: (i // CHUNK, i % CHUNK) for i, block in enumerate(BLOCKS)}


def exchange(
    sections, ranks, k_ref, v_ref, g_ref, out_ref, scale_ref,
    raw, gain, scaled, rows_out, rows_in, rows_at,
    load_sem, gain_sem, send_sem, recv_sem, row_send_sem, row_recv_sem, plane_sem, rest_sem,
):
    devices = sections * ranks
    section, rank = lax.axis_index("section"), lax.axis_index("tensor")
    me = section * ranks + rank
    model_rows = k_ref.shape[1]
    part = model_rows // sections
    share = part // ranks
    blocks = part // BLOCK
    core, my_x = section % 2, section // 2 % SIDE
    my_y, my_z = rank // SIDE * 2 + section // (2 * SIDE), rank % SIDE
    toward = 1 - 2 * (my_z % 2)

    def target(offset):
        x, y = (my_x + offset[0]) % SIDE, (my_y + offset[1]) % SIDE
        z = (my_z + toward * offset[2] + SIDE) % SIDE
        return (y % 2 * SIDE + x) * 2 + (core + offset[3]) % 2, y // 2 * SIDE + z

    def block_at(block):
        there, other = target(block[:2] + (block[2] * 2, block[3]))
        return there, other // 2

    def load(chunk):
        for place, block in enumerate(CHUNKS[chunk]):
            there, inner = block_at(block)
            rows = pl.ds(pl.multiple_of(there * part + inner * BLOCK, BLOCK), BLOCK)
            for kind, ref in enumerate((k_ref, v_ref)):
                pltpu.make_async_copy(
                    ref.at[0, rows], raw.at[(chunk * 2 + kind) * CHUNK + place], load_sem.at[chunk]
                ).start()

    lanes = lax.broadcasted_iota(jnp.int32, (1, BLOCK), 1)

    def compute(chunk):
        if chunk + AHEAD < len(CHUNKS):
            load(chunk + AHEAD)
        here = raw.at[pl.ds(chunk * 2 * CHUNK, 2 * CHUNK)]
        pltpu.make_async_copy(here, here, load_sem.at[chunk]).wait()
        for place, block in enumerate(CHUNKS[chunk]):
            there, inner = block_at(block)
            start = pl.multiple_of(there * part + inner * BLOCK, BLOCK)
            gain_rows = gain[:, pl.ds(start, BLOCK)].astype(jnp.float32)
            gain_rows = jnp.broadcast_to(gain_rows, (BLOCK, BLOCK)).T
            row_values = rows_out[there]
            for kind in range(2):
                folded = gain_rows * raw[(chunk * 2 + kind) * CHUNK + place].astype(jnp.float32)
                folded = folded.astype(jnp.bfloat16).astype(jnp.float32)
                peak = jnp.max(jnp.abs(folded), axis=(0, 1), keepdims=True)
                peak = jnp.maximum(peak, SCALE_FLOOR)
                scaled[chunk, place, kind] = (folded * (1.0 / peak)).astype(jnp.bfloat16)
                lane = (kind * sections + section) * blocks + inner
                row_values = jnp.where(lanes == lane, peak, row_values)
            rows_out[there] = row_values

    columns = pl.ds(pl.multiple_of(rank * BLOCK, BLOCK), BLOCK)

    def piece(offset):
        there, other = target(offset)
        chunk, place = PLACE[block_of(offset)]
        half = pl.multiple_of(other % 2 * share, share)
        return there, other, scaled.at[chunk, place, :, pl.ds(half, share)]

    def send(offset):
        there, other, source = piece(offset)
        pltpu.make_async_remote_copy(
            src_ref=source,
            dst_ref=out_ref.at[section, :, :, columns],
            send_sem=send_sem,
            recv_sem=recv_sem,
            device_id=(there, other),
            device_id_type=MESH,
        ).start()

    def greet(semaphore, peers):
        for offset in peers:
            pl.semaphore_signal(
                semaphore, inc=1, device_id=target(offset), device_id_type=MESH
            )

    done = 0

    def send_group(group, done):
        for offset in group:
            while PLACE[block_of(offset)][0] >= done:
                compute(done)
                done += 1
            send(offset)
        return done

    barrier = pltpu.get_barrier_semaphore()
    gain_copy = pltpu.make_async_copy(g_ref, gain, gain_sem)
    gain_copy.start()
    load(0)
    greet(barrier, LINES)
    for chunk in range(1, AHEAD):
        load(chunk)
    rows_out[...] = jnp.zeros_like(rows_out)
    gain_copy.wait()
    compute(0)
    compute(1)
    done = 2
    pl.semaphore_wait(barrier, len(LINES))
    greet(plane_sem, SAME_CORE)
    done = send_group(LINES, done)
    pl.semaphore_wait(plane_sem, len(SAME_CORE))
    greet(rest_sem, ALONG_X)
    done = send_group(PLANES[:36], done)
    while done < len(CHUNKS):
        compute(done)
        done += 1
    pl.semaphore_wait(rest_sem, len(ALONG_X))

    def send_row(source, landing, there, other, stage):
        pltpu.make_async_remote_copy(
            src_ref=source,
            dst_ref=landing,
            send_sem=row_send_sem.at[stage],
            recv_sem=row_recv_sem.at[stage],
            device_id=(there, other),
            device_id_type=MESH,
        ).start()

    def wait_rows(semaphores, stage, count):
        some = rows_in.at[pl.ds(0, count)]
        pltpu.make_async_copy(some, some, semaphores.at[stage]).wait()

    @pl.loop(1, sections)
    def _(step):
        there = lax.rem(section + step, sections)
        send_row(rows_out.at[there], rows_in.at[section], there, rank, 0)

    send_group(REST + PLANES[36:], done)
    rows_in[section] = rows_out[section]
    wait_rows(row_recv_sem, 0, sections - 1)
    rows_at[rank] = jnp.max(rows_in[...], axis=0)
    out_ref[section, :, :, columns] = piece((0, 0, 0, 0))[2][...]

    @pl.loop(1, ranks)
    def _(step):
        other = lax.rem(rank + step, ranks)
        send_row(rows_at.at[rank], rows_at.at[rank], section, other, 1)

    wait_rows(row_recv_sem, 1, ranks - 1)
    by_rank = jnp.concatenate([rows_at[other] for other in range(ranks)] * (BLOCK // ranks), axis=0).T
    first_half, second_half = by_rank[: BLOCK // 2], by_rank[BLOCK // 2 :]
    all_scales = jnp.where(lanes < ranks, first_half, second_half)
    for layer in range(sections):
        scale_ref[layer] = all_scales[layer * blocks : (layer + 1) * blocks, : 2 * ranks]

    pieces = raw.at[pl.ds(0, devices - 1)]
    pltpu.make_async_copy(pieces, pieces, recv_sem).wait()
    wait_rows(row_send_sem, 0, sections - 1)
    wait_rows(row_send_sem, 1, ranks - 1)
    pltpu.make_async_copy(pieces, pieces, send_sem).wait()


def settle(wide_ref, narrow_ref, scaled_ref, scale_ref, sem, scale_sem):
    layers, kinds, _, columns = wide_ref.shape
    copies = [
        pltpu.make_async_copy(
            wide_ref.at[layer, kind],
            scaled_ref.at[layer, :, pl.ds(kind * columns, columns)],
            sem.at[layer, kind],
        )
        for layer in range(layers)
        for kind in range(kinds)
    ]
    copies.append(pltpu.make_async_copy(narrow_ref, scale_ref, scale_sem))
    for copy in copies:
        copy.start()
    for copy in copies:
        copy.wait()


def on_device(key_weight, value_weight, norm_gain):
    sections, ranks = lax.axis_size("section"), lax.axis_size("tensor")
    devices = sections * ranks
    model_rows = key_weight.shape[1]
    share = model_rows // devices
    blocks = model_rows // sections // BLOCK
    anywhere = pl.BlockSpec(memory_space=pl.ANY)
    in_vmem = pl.BlockSpec(memory_space=pltpu.VMEM)
    in_space = pltpu.with_memory_space_constraint
    wide, narrow = pl.pallas_call(
        functools.partial(exchange, sections, ranks),
        out_shape=(
            pltpu.VMEM((sections, 2, share, ranks * BLOCK), jnp.bfloat16),
            pltpu.VMEM((sections, blocks, 2 * ranks), jnp.float32),
        ),
        in_specs=[anywhere] * 3,
        out_specs=(in_vmem, in_vmem),
        scratch_shapes=[
            pltpu.VMEM((len(BLOCKS) * 2, BLOCK, BLOCK), jnp.bfloat16),
            pltpu.VMEM((1, model_rows), jnp.bfloat16),
            pltpu.VMEM((len(CHUNKS), CHUNK, 2, BLOCK, BLOCK), jnp.bfloat16),
            pltpu.VMEM((sections, 1, BLOCK), jnp.float32),
            pltpu.VMEM((sections, 1, BLOCK), jnp.float32),
            pltpu.VMEM((ranks, 1, BLOCK), jnp.float32),
            pltpu.SemaphoreType.DMA((len(CHUNKS),)),
            pltpu.SemaphoreType.DMA,
            pltpu.SemaphoreType.DMA,
            pltpu.SemaphoreType.DMA,
            pltpu.SemaphoreType.DMA((2,)),
            pltpu.SemaphoreType.DMA((2,)),
            pltpu.SemaphoreType.REGULAR,
            pltpu.SemaphoreType.REGULAR,
        ],
        compiler_params=pltpu.CompilerParams(
            collective_id=0, has_side_effects=True, vmem_limit_bytes=32 * 1024 * 1024
        ),
    )(*(in_space(array, pltpu.HBM) for array in (key_weight, value_weight, norm_gain)))
    return pl.pallas_call(
        settle,
        out_shape=(
            jax.ShapeDtypeStruct((sections, share, 2 * ranks * BLOCK), jnp.bfloat16),
            jax.ShapeDtypeStruct(narrow.shape, jnp.float32),
        ),
        in_specs=[in_vmem, in_vmem],
        out_specs=(anywhere, anywhere),
        scratch_shapes=[
            pltpu.SemaphoreType.DMA((sections, 2)),
            pltpu.SemaphoreType.DMA,
        ],
        compiler_params=pltpu.CompilerParams(vmem_limit_bytes=4 * 1024 * 1024),
    )(in_space(wide, pltpu.VMEM), in_space(narrow, pltpu.VMEM))


def solution(mesh):
    placed = (P("section", None, "tensor"), P("section", None, "tensor"), P("section", None))
    return jax.shard_map(
        on_device,
        mesh=mesh,
        in_specs=placed,
        out_specs=(P(None, ("section", "tensor"), None), P(None, "section", None)),
        check_vma=False,
    )
```
